32 devices in a mesh: dp: 1 (over z), ep2: 4 (over y), ep: 8 (over x, core).
Axes of the slice: x: 4, y: 4, z: 1, core: 2. Of those that a mesh axis runs over, the one named last changes fastest.
The devices are a block of a 4x4x8 slice.
Arguments:
- tokens: bfloat16 [4096, 2560], P(('dp', 'ep2', 'ep'))
- expert_ids: int32 [4096, 6], P(('dp', 'ep2', 'ep'))
- gates: float32 [4096, 6], P(('dp', 'ep2', 'ep'))
- w_gate: bfloat16 [64, 2560, 1536], P(('ep2', 'ep'))
- w_up: bfloat16 [64, 2560, 1536], P(('ep2', 'ep'))
- w_down: bfloat16 [64, 1536, 2560], P(('ep2', 'ep'))
Outputs:
- output: bfloat16 [4096, 2560], P(('dp', 'ep2', 'ep'))
All inputs are finite; a program needn't handle non-finite values.
Results may differ from the reference program's by a relative error of at most 0.001.
Values are sent between devices in bfloat16 or wider.
A program may use at most 768 MiB of HBM per device.

```python
import jax
import jax.numpy as jnp
from jax import lax

MODEL_DIM = 2560
FFN_DIM = 1536
NUM_EXPERTS = 64
TOP_K = 6
TOK_DEV = 128
GROUP_DEVS = 32


def random_perms(perm_key, n_rows, length):
    scores = jax.random.randint(perm_key, (n_rows, length), 0, 1048576) * length + jnp.arange(length)[None, :]
    return jnp.argsort(scores, axis=1, stable=True)


def draw_routing(route_key):
    local_count = NUM_EXPERTS // GROUP_DEVS
    key_dev, key_loc, key_tok, key_off = jax.random.split(route_key, 4)
    dev_perm = random_perms(key_dev, GROUP_DEVS, GROUP_DEVS)
    loc_perm = random_perms(key_loc, GROUP_DEVS, local_count)
    tok_perm = random_perms(key_tok, GROUP_DEVS, TOK_DEV)
    offset = jax.random.randint(key_off, (GROUP_DEVS, 1, 1), 0, NUM_EXPERTS)
    row_pos = offset + tok_perm[:, :, None] * TOP_K + jnp.arange(TOP_K)[None, None, :]
    row_mod = (row_pos % NUM_EXPERTS).reshape(GROUP_DEVS, TOK_DEV * TOP_K)
    dev_col = row_mod % GROUP_DEVS
    loc_col = row_mod // GROUP_DEVS
    dest_dev = jnp.take_along_axis(dev_perm, dev_col, axis=1)
    dest_loc = (jnp.take_along_axis(loc_perm, loc_col, axis=1) + dev_col) % local_count
    expert_ids = dest_dev * local_count + dest_loc
    return expert_ids.reshape(GROUP_DEVS * TOK_DEV, TOP_K).astype(jnp.int32)


def setup_inputs(seed: int = 0, part: int = 0) -> dict:
    base_key = jax.random.key(seed)
    part_key = jax.random.fold_in(base_key, part)
    key_x, key_route, key_gate = jax.random.split(part_key, 3)
    key_w1, key_w3, key_w2 = jax.random.split(base_key, 3)
    n_tok = GROUP_DEVS * TOK_DEV
    tokens = jax.random.normal(key_x, (n_tok, MODEL_DIM), jnp.float32).astype(jnp.bfloat16)
    expert_ids = draw_routing(key_route)
    gates = jax.nn.softmax(1.5 * jax.random.normal(key_gate, (n_tok, TOP_K), jnp.float32), axis=-1)
    w_gate = (jax.random.normal(key_w1, (NUM_EXPERTS, MODEL_DIM, FFN_DIM), jnp.float32) * MODEL_DIM ** -0.5).astype(jnp.bfloat16)
    w_up = (jax.random.normal(key_w3, (NUM_EXPERTS, MODEL_DIM, FFN_DIM), jnp.float32) * MODEL_DIM ** -0.5).astype(jnp.bfloat16)
    w_down = (jax.random.normal(key_w2, (NUM_EXPERTS, FFN_DIM, MODEL_DIM), jnp.float32) * (3.0 * FFN_DIM ** -0.5)).astype(jnp.bfloat16)
    return {'tokens': tokens, 'expert_ids': expert_ids, 'gates': gates, 'w_gate': w_gate, 'w_up': w_up, 'w_down': w_down}


def expert_rows(operands):
    rows, w_one, w_three, w_two = operands
    act_gate = jnp.dot(rows, w_one, preferred_element_type=jnp.float32)
    act_up = jnp.dot(rows, w_three, preferred_element_type=jnp.float32)
    hidden = (jax.nn.silu(act_gate) * act_up).astype(jnp.bfloat16)
    return jnp.dot(hidden, w_two, preferred_element_type=jnp.float32).astype(jnp.bfloat16)


def reference(tokens, expert_ids, gates, w_gate, w_up, w_down):
    n_tok = tokens.shape[0]
    n_rows = n_tok * TOP_K
    per_expert = GROUP_DEVS * ((TOK_DEV * TOP_K + NUM_EXPERTS - 1) // NUM_EXPERTS)
    flat_ids = expert_ids.reshape(n_rows)
    sort_order = jnp.argsort(flat_ids, stable=True)
    counts = jnp.bincount(flat_ids, length=NUM_EXPERTS)
    starts = jnp.cumsum(counts) - counts
    rank_sorted = (jnp.arange(n_rows) - starts[flat_ids[sort_order]]).astype(jnp.int32)
    row_rank = jnp.zeros((n_rows,), jnp.int32).at[sort_order].set(rank_sorted)
    dest_pos = flat_ids * per_expert + row_rank
    buffer = jnp.zeros((NUM_EXPERTS * per_expert, MODEL_DIM), tokens.dtype).at[dest_pos].set(jnp.repeat(tokens, TOP_K, axis=0))
    expert_out = lax.map(expert_rows, (buffer.reshape(NUM_EXPERTS, per_expert, MODEL_DIM), w_gate, w_up, w_down))
    picked = expert_out.reshape(NUM_EXPERTS * per_expert, MODEL_DIM)[dest_pos].reshape(n_tok, TOP_K, MODEL_DIM)
    total = tokens.astype(jnp.float32)
    for slot_j in range(TOP_K):
        total = total + gates[:, slot_j:slot_j + 1] * picked[:, slot_j].astype(jnp.float32)
    return total.astype(jnp.bfloat16)
```

```python
import functools

import jax
import jax.numpy as jnp
from jax import lax
from jax.experimental import pallas as pl
from jax.experimental.pallas import tpu as pltpu
from jax.sharding import PartitionSpec as P

MESH = pl.DeviceIdType.MESH
F32 = jnp.float32
BF16 = jnp.bfloat16
PEERS = [(1, 0), (3, 0), (1, 1), (3, 1), (2, 0), (2, 1), (0, 1)]
MATES = [1, 3, 2]


def div12(v):
    return (v * 2731) >> 15


def nt_dot(a, b):
    return lax.dot_general(a, b, (((1,), (1,)), ((), ())), preferred_element_type=F32)


def dot(a, b):
    return jnp.dot(a, b, preferred_element_type=F32)


def moe_kernel(
    n_line, cap, n_half, n_chunk, f_tile,
    x_ref, idx_ref, gate_ref, w1_hbm, w3_hbm, w2_hbm, out_ref,
    w1, w3, w2, mts, m_own, xg, sel, sendb, rows, hid, y1, y3, perm, gmat, acc,
    w13_sem, w2_sem, mt_s, mt_r, g_s, g_r, d_s, d_r, c_s, c_r, e_s, e_r,
):
    n_tok, dim = x_ref.shape
    n_top = idx_ref.shape[1]
    n_loc, ffn = w2_hbm.shape[0], w2_hbm.shape[1]
    n_exp = mts.shape[1]
    per = n_line * cap
    n_rows = 2 * n_line * per
    n_w2 = w2.shape[0]
    half = dim // n_half
    wide = dim // n_chunk

    dp = lax.axis_index('dp')
    yy = lax.axis_index('ep2')
    ee = lax.axis_index('ep')
    xx = ee // 2
    cc = lax.rem(ee, 2)
    k_self = jnp.where(cc == 0, yy, xx)
    q_self = jnp.where(cc == 0, xx, yy)
    i_self = cc * n_line + q_self
    d_self = 2 * q_self + cc
    coef_k = jnp.where(cc == 0, 16, 4)
    coef_q = jnp.where(cc == 0, 4, 16)

    def mod(v):
        return lax.rem(v + n_line, n_line)

    def mate(m):
        k = mod(k_self + m)
        return (dp, jnp.where(cc == 0, k, yy), jnp.where(cc == 0, xx, k) * 2 + cc)

    def spread_peer(m, dc):
        q = mod(q_self + m)
        c2 = lax.rem(cc + dc, 2)
        dev = (dp, jnp.where(cc == 0, yy, q), jnp.where(cc == 0, q, xx) * 2 + c2)
        return dev, 2 * q + c2

    def rows_at(start, size, unit):
        return pl.ds(pl.multiple_of(start, unit), size)

    def half_cols(h):
        return pl.ds(h * half, half)

    def cols_at(c):
        return pl.ds(pl.multiple_of(c * wide, wide), wide)

    def w13_copy(which, l):
        hbm, buf = ((w1_hbm, w1), (w3_hbm, w3))[which]
        return pltpu.make_async_copy(hbm.at[l], buf.at[l], w13_sem.at[which, l])

    def w2_copy(t):
        slot = lax.rem(t, n_w2)
        return pltpu.make_async_copy(
            w2_hbm.at[t // n_chunk, :, cols_at(lax.rem(t, n_chunk))], w2.at[slot], w2_sem.at[slot])

    def mt_copy(m):
        return pltpu.make_async_remote_copy(
            mts.at[k_self], mts.at[k_self], mt_s.at[m - 1], mt_r.at[m - 1], device_id=mate(m), device_id_type=MESH)

    def gather_copy(m, h):
        return pltpu.make_async_remote_copy(
            x_ref.at[:, half_cols(h)], xg.at[rows_at(k_self * n_tok, n_tok, 8), half_cols(h)],
            g_s.at[m - 1, h], g_r.at[m - 1, h], device_id=mate(m), device_id_type=MESH)

    def spread_copy(l, h, m, dc):
        dev, d = spread_peer(m, dc)
        return pltpu.make_async_remote_copy(
            sendb.at[l, rows_at(d * per, per, 8), half_cols(h)],
            rows.at[l, rows_at(i_self * per, per, 8), half_cols(h)],
            d_s.at[l, h, d], d_r.at[l, h, i_self], device_id=dev, device_id_type=MESH)

    def spread_wait(l, h):
        for o in range(1, 2 * n_line):
            i = lax.rem(i_self + o, 2 * n_line)
            pltpu.make_async_remote_copy(
                sendb.at[l, rows_at(i * per, per, 8), half_cols(h)],
                rows.at[l, rows_at(i * per, per, 8), half_cols(h)],
                d_s.at[l, h, i], d_r.at[l, h, i], device_id=mate(1), device_id_type=MESH).wait_recv()

    def back_targets():
        out = []
        for m in (1, 3, 2):
            for side in (0, 1):
                pos = mod((yy if side else xx) + m)
                dev = (dp, pos, xx * 2 + 1) if side else (dp, yy, pos * 2)
                d_me = 2 * (yy if side else xx) + cc
                out.append((side * n_line + pos, dev, d_me))
        other = 1 - cc
        pos = jnp.where(other == 0, xx, yy)
        out.append((other * n_line + pos, (dp, yy, xx * 2 + other), 2 * pos + cc))
        return out

    def back_copies(l, c):
        return [
            pltpu.make_async_remote_copy(
                rows.at[l, rows_at(i * per, per, 8), cols_at(c)], y1.at[l, rows_at(d_me * per, per, 8), cols_at(c)],
                c_s.at[l, c, i], c_r.at[l, c, d_me], device_id=dev, device_id_type=MESH)
            for i, dev, d_me in back_targets()
        ]

    def back_wait(l, c):
        for o in range(1, 2 * n_line):
            d = lax.rem(d_self + o, 2 * n_line)
            pltpu.make_async_remote_copy(
                rows.at[l, rows_at(d * per, per, 8), cols_at(c)], y1.at[l, rows_at(d * per, per, 8), cols_at(c)],
                c_s.at[l, c, d], c_r.at[l, c, d], device_id=mate(1), device_id_type=MESH).wait_recv()

    home = 2 * n_line * cap

    def home_copy(l, c, m):
        s = mod(k_self + m)
        return pltpu.make_async_remote_copy(
            sendb.at[l, rows_at(s * home, home, 8), cols_at(c)], y3.at[l, rows_at(k_self * home, home, 8), cols_at(c)],
            e_s.at[l, c, m - 1], e_r.at[l, c, m - 1], device_id=mate(m), device_id_type=MESH)

    for l in range(n_loc):
        for which in range(2):
            w13_copy(which, l).start()
    for t in range(n_w2):
        w2_copy(t).start()

    barrier = pltpu.get_barrier_semaphore()
    for side in (0, 1):
        for m in range(n_line):
            for dc in (0, 1):
                if (m, dc) == (0, 0) or (side and m == 0):
                    continue
                pos = mod((yy if side else xx) + m)
                c2 = lax.rem(cc + dc, 2)
                dev = (dp, pos, xx * 2 + c2) if side else (dp, yy, pos * 2 + c2)
                pl.semaphore_signal(barrier, inc=1, device_id=dev, device_id_type=MESH)

    lane_e = lax.broadcasted_iota(jnp.int32, (n_tok, n_exp), 1)
    chosen = jnp.zeros((n_tok, n_exp), F32)
    for j in range(n_top):
        chosen = chosen + (idx_ref[:, j:j + 1] == lane_e).astype(F32)
    lower = (lax.broadcasted_iota(jnp.int32, (n_tok, n_tok), 1)
             < lax.broadcasted_iota(jnp.int32, (n_tok, n_tok), 0)).astype(BF16)
    slot = dot(lower, chosen.astype(BF16))
    slot = jnp.where(chosen > 0, slot, -1.0).astype(BF16)
    m_own[...] = slot
    eye = (lax.broadcasted_iota(jnp.int32, (n_exp, n_exp), 0)
           == lax.broadcasted_iota(jnp.int32, (n_exp, n_exp), 1)).astype(BF16)
    mts[k_self] = nt_dot(eye, slot).astype(BF16)

    pl.semaphore_wait(barrier, 4 * n_line - 3)

    for m in MATES:
        mt_copy(m).start()
    for h in range(n_half):
        for m in MATES:
            gather_copy(m, h).start()

    xg[rows_at(k_self * n_tok, n_tok, 8), :] = x_ref[...]

    r = lax.broadcasted_iota(jnp.int32, (n_rows, 1), 0)
    r12 = div12(r)
    r_slot = (r - r12 * cap).astype(F32)
    r_src = r12 & (n_line - 1)
    r_dev = r12 >> 2
    r_exp0 = coef_k * k_self + coef_q * (r_dev >> 1) + 2 * (r_dev & 1)
    e_lane = lax.broadcasted_iota(jnp.int32, (n_rows, n_exp), 1)
    for m in MATES:
        mt_copy(m).wait_recv()
    for l in range(n_loc):
        pick = (e_lane == r_exp0 + l).astype(BF16)
        for s in range(n_line):
            val = dot(pick, mts[s])
            hit = jnp.logical_and(val == r_slot, r_src == s)
            sel[l, :, s * n_tok:(s + 1) * n_tok] = jnp.where(hit, 1.0, 0.0).astype(BF16)

    def spread(l, h):
        sendb[l, :, half_cols(h)] = dot(sel[l], xg[:, half_cols(h)]).astype(BF16)
        for m, dc in PEERS:
            spread_copy(l, h, m, dc).start()
        rows[l, rows_at(i_self * per, per, 8), half_cols(h)] = sendb[l, rows_at(d_self * per, per, 8), half_cols(h)]

    for h in range(n_half):
        for m in MATES:
            gather_copy(m, h).wait_recv()
        spread(0, h)
    for h in range(n_half):
        for l in range(1, n_loc):
            spread(l, h)

    o12 = r12
    o_in = (o12 & 7) * per + (o12 >> 3) * cap + (r - r12 * cap)
    perm[...] = (lax.broadcasted_iota(jnp.int32, (n_rows, n_rows), 1) == o_in).astype(BF16)

    gate = jnp.zeros((n_tok, n_exp), F32)
    for j in range(n_top):
        gate = gate + jnp.where(idx_ref[:, j:j + 1] == lane_e, gate_ref[:, j:j + 1], 0.0)
    parts = []
    rest = gate
    for _ in range(3):
        part = rest.astype(BF16)
        parts.append(part)
        rest = rest - part.astype(F32)
    q = lax.broadcasted_iota(jnp.int32, (1, n_rows), 1)
    q12 = div12(q)
    q_slot = (q - q12 * cap).astype(F32)
    q_dev = q12 & 7
    q_exp0 = coef_k * (q12 >> 3) + coef_q * (q_dev >> 1) + 2 * (q_dev & 1)
    e_row = lax.broadcasted_iota(jnp.int32, (n_exp, n_rows), 0)
    for l in range(n_loc):
        spread_e = (e_row == q_exp0 + l).astype(BF16)
        hit = dot(m_own[...], spread_e) == q_slot
        for p in range(3):
            gmat[l, p * n_tok:(p + 1) * n_tok, :] = jnp.where(hit, dot(parts[p], spread_e), 0.0).astype(BF16)
    acc[...] = x_ref[...].astype(F32)

    def expert_up(l):
        for h in range(n_half):
            spread_wait(l, h)
        for which in range(2):
            w13_copy(which, l).wait()

        def tile(n, carry):
            cols = pl.ds(pl.multiple_of(n * f_tile, f_tile), f_tile)
            a = dot(rows[l], w1[l, :, cols])
            b = dot(rows[l], w3[l, :, cols])
            hid[:, cols] = (jax.nn.silu(a) * b).astype(BF16)
            return carry

        lax.fori_loop(0, ffn // f_tile, tile, 0)

    def expert_down(l, c):
        t = l * n_chunk + c
        w2_copy(t).wait()
        rows[l, :, cols_at(c)] = dot(hid[...], w2[lax.rem(t, n_w2)]).astype(BF16)

        @pl.when(t + n_w2 < n_loc * n_chunk)
        def _():
            w2_copy(t + n_w2).start()

        for copy in back_copies(l, c):
            copy.start()
        y1[l, rows_at(d_self * per, per, 8), cols_at(c)] = rows[l, rows_at(i_self * per, per, 8), cols_at(c)]

    def forward(l, c):
        back_wait(l, c)
        sendb[l, :, cols_at(c)] = dot(perm[...], y1[l, :, cols_at(c)]).astype(BF16)
        for m in MATES:
            home_copy(l, c, m).start()
        y3[l, rows_at(k_self * home, home, 8), cols_at(c)] = sendb[l, rows_at(k_self * home, home, 8), cols_at(c)]

    def collect(l, c):
        for m in MATES:
            home_copy(l, c, m).wait_recv()
        part = dot(gmat[l], y3[l, :, cols_at(c)])
        acc[:, cols_at(c)] += part[:n_tok] + part[n_tok:2 * n_tok] + part[2 * n_tok:]

    def loop(body):
        def step(c, carry):
            body(c)
            return carry
        lax.fori_loop(0, n_chunk, step, 0)

    expert_up(0)
    loop(lambda c: expert_down(0, c))
    expert_up(1)
    for l in range(n_loc):
        for h in range(n_half):
            for m, dc in PEERS:
                spread_copy(l, h, m, dc).wait_send()

    def down_and_forward(c):
        expert_down(1, c)
        forward(0, c)

    loop(down_and_forward)

    def forward_and_collect(c):
        forward(1, c)
        collect(0, c)

    loop(forward_and_collect)

    def finish(c):
        collect(1, c)
        out_ref[:, cols_at(c)] = acc[:, cols_at(c)].astype(BF16)

    loop(finish)

    for m in MATES:
        mt_copy(m).wait_send()
        for h in range(n_half):
            gather_copy(m, h).wait_send()

    def drain(c):
        for l in range(n_loc):
            for copy in back_copies(l, c):
                copy.wait_send()
            for m in MATES:
                home_copy(l, c, m).wait_send()

    loop(drain)


def solution(mesh):
    group_axes = ('ep2', 'ep')
    n_line = mesh.shape['ep2']
    n_group = n_line * mesh.shape['ep']
    row_spec = P(('dp', 'ep2', 'ep'), None)
    weight_spec = P(group_axes, None, None)

    def device_step(tokens, expert_ids, gates, w_gate, w_up, w_down):
        n_tok, n_top = expert_ids.shape
        n_loc, dim, ffn = w_gate.shape
        n_exp = n_loc * n_group
        cap = -(-(n_tok * n_top) // n_exp)
        n_rows = n_group * cap
        n_half, n_chunk, f_tile, n_w2 = 2, 5, 256, 4
        sem = pltpu.SemaphoreType.DMA
        vmem = pl.BlockSpec(memory_space=pltpu.VMEM)
        hbm = pl.BlockSpec(memory_space=pl.ANY)
        n_dev = 2 * n_line
        return pl.pallas_call(
            functools.partial(moe_kernel, n_line, cap, n_half, n_chunk, f_tile),
            out_shape=jax.ShapeDtypeStruct((n_tok, dim), BF16),
            in_specs=[vmem, vmem, vmem, hbm, hbm, hbm],
            out_specs=vmem,
            scratch_shapes=[
                pltpu.VMEM((n_loc, dim, ffn), BF16),
                pltpu.VMEM((n_loc, dim, ffn), BF16),
                pltpu.VMEM((n_w2, ffn, dim // n_chunk), BF16),
                pltpu.VMEM((n_line, n_exp, n_tok), BF16),
                pltpu.VMEM((n_tok, n_exp), BF16),
                pltpu.VMEM((n_line * n_tok, dim), BF16),
                pltpu.VMEM((n_loc, n_rows, n_line * n_tok), BF16),
                pltpu.VMEM((n_loc, n_rows, dim), BF16),
                pltpu.VMEM((n_loc, n_rows, dim), BF16),
                pltpu.VMEM((n_rows, ffn), BF16),
                pltpu.VMEM((n_loc, n_rows, dim), BF16),
                pltpu.VMEM((n_loc, n_rows, dim), BF16),
                pltpu.VMEM((n_rows, n_rows), BF16),
                pltpu.VMEM((n_loc, 3 * n_tok, n_rows), BF16),
                pltpu.VMEM((n_tok, dim), F32),
                sem((2, n_loc)),
                sem((n_w2,)),
                sem((n_line - 1,)), sem((n_line - 1,)),
                sem((n_line - 1, n_half)), sem((n_line - 1, n_half)),
                sem((n_loc, n_half, n_dev)), sem((n_loc, n_half, n_dev)),
                sem((n_loc, n_chunk, n_dev)), sem((n_loc, n_chunk, n_dev)),
                sem((n_loc, n_chunk, n_line - 1)), sem((n_loc, n_chunk, n_line - 1)),
            ],
            compiler_params=pltpu.CompilerParams(
                collective_id=0, has_side_effects=True, vmem_limit_bytes=67043328),
        )(tokens, expert_ids, gates, w_gate, w_up, w_down)

    return jax.shard_map(
        device_step, mesh=mesh,
        in_specs=(row_spec, row_spec, row_spec, weight_spec, weight_spec, weight_spec),
        out_specs=row_spec, check_vma=False)
```

```python
import functools

import jax
import jax.numpy as jnp
from jax import lax
from jax.experimental import pallas as pl
from jax.experimental.pallas import tpu as pltpu
from jax.sharding import PartitionSpec as P

MESH = pl.DeviceIdType.MESH
F32 = jnp.float32
BF16 = jnp.bfloat16
PEERS = [(1, 0), (3, 0), (1, 1), (3, 1), (2, 0), (2, 1), (0, 1)]
MATES = [1, 3, 2]


def div12(v):
    return (v * 2731) >> 15


def nt_dot(a, b):
    return lax.dot_general(a, b, (((1,), (1,)), ((), ())), preferred_element_type=F32)


def dot(a, b):
    return jnp.dot(a, b, preferred_element_type=F32)


def moe_kernel(
    n_line, cap, n_half, n_chunk, f_tile, cuts, ahead, lead,
    x_hbm, idx_hbm, gate_hbm, w1_hbm, w3_hbm, w2_hbm, out_ref,
    x_ref, idx_ref, gate_ref, w1, w3, w2, mts, xg, sel, sendb, rows, part_a, part_b, hid, y1, y3, perm, gmat, acc,
    in_sem, w13_sem, w2_sem, mt_s, mt_r, g_s, g_r, d_s, d_r, c_s, c_r, e_s, e_r,
):
    n_tok, dim = x_ref.shape
    n_top = idx_ref.shape[0]
    n_loc, ffn = w2_hbm.shape[0], w2_hbm.shape[1]
    n_exp = mts.shape[1]
    per = n_line * cap
    n_rows = 2 * n_line * per
    n_w2 = w2.shape[0]
    half = dim // n_half
    wide = dim // n_chunk

    dp = lax.axis_index('dp')
    yy = lax.axis_index('ep2')
    ee = lax.axis_index('ep')
    xx = ee // 2
    cc = lax.rem(ee, 2)
    k_self = jnp.where(cc == 0, yy, xx)
    q_self = jnp.where(cc == 0, xx, yy)
    i_self = cc * n_line + q_self
    d_self = 2 * q_self + cc
    coef_k = jnp.where(cc == 0, 16, 4)
    coef_q = jnp.where(cc == 0, 4, 16)

    def mod(v):
        return lax.rem(v + n_line, n_line)

    def mate(m):
        k = mod(k_self + m)
        return (dp, jnp.where(cc == 0, k, yy), jnp.where(cc == 0, xx, k) * 2 + cc)

    def spread_peer(m, dc):
        q = mod(q_self + m)
        c2 = lax.rem(cc + dc, 2)
        dev = (dp, jnp.where(cc == 0, yy, q), jnp.where(cc == 0, q, xx) * 2 + c2)
        return dev, 2 * q + c2

    def rows_at(start, size, unit):
        return pl.ds(pl.multiple_of(start, unit), size)

    def half_cols(h):
        return pl.ds(h * half, half)

    def cols_at(c):
        return pl.ds(pl.multiple_of(c * wide, wide), wide)

    def w13_copy(which, l):
        hbm, buf = ((w1_hbm, w1), (w3_hbm, w3))[which]
        return pltpu.make_async_copy(hbm.at[l], buf.at[l], w13_sem.at[which, l])

    def w2_copy(t):
        slot = lax.rem(t, n_w2)
        return pltpu.make_async_copy(
            w2_hbm.at[t // n_chunk, :, cols_at(lax.rem(t, n_chunk))], w2.at[slot], w2_sem.at[slot])

    def mt_copy(m):
        return pltpu.make_async_remote_copy(
            mts.at[k_self], mts.at[k_self], mt_s.at[0], mt_r.at[0], device_id=mate(m), device_id_type=MESH)

    def gather_copy(m, h):
        return pltpu.make_async_remote_copy(
            x_ref.at[:, half_cols(h)], xg.at[rows_at(k_self * n_tok, n_tok, 8), half_cols(h)],
            g_s.at[0], g_r.at[m // 2, h], device_id=mate(m), device_id_type=MESH)

    def relay_copy(m, h):
        side = m // 2
        block = xg.at[rows_at(mod(k_self - m) * n_tok + side * (n_tok // 2), n_tok // 2, 8), half_cols(h)]
        return pltpu.make_async_remote_copy(
            block, block, g_s.at[0], g_r.at[2 + side, h], device_id=mate(m), device_id_type=MESH)

    def wait_bytes(ref, sem):
        pltpu.make_async_copy(ref, ref, sem).wait()

    def spread_copy(l, h, m, dc):
        dev, d = spread_peer(m, dc)
        return pltpu.make_async_remote_copy(
            sendb.at[l, rows_at(d * per, per, 8), half_cols(h)],
            rows.at[l, rows_at(i_self * per, per, 8), half_cols(h)],
            d_s.at[0], d_r.at[l, h], device_id=dev, device_id_type=MESH)

    others = (2 * n_line - 1) * per

    def spread_wait(l, h):
        wait_bytes(rows.at[l, pl.ds(0, others), half_cols(h)], d_r.at[l, h])

    def back_targets():
        out = []
        for m in (1, 3, 2):
            for side in (0, 1):
                pos = mod((yy if side else xx) + m)
                dev = (dp, pos, xx * 2 + 1) if side else (dp, yy, pos * 2)
                d_me = 2 * (yy if side else xx) + cc
                out.append((side * n_line + pos, dev, d_me))
        other = 1 - cc
        pos = jnp.where(other == 0, xx, yy)
        out.append((other * n_line + pos, (dp, yy, xx * 2 + other), 2 * pos + cc))
        return out

    def back_copies(l, c):
        return [
            pltpu.make_async_remote_copy(
                rows.at[l, rows_at(i * per, per, 8), cols_at(c)], y1.at[l, rows_at(d_me * per, per, 8), cols_at(c)],
                c_s.at[0], c_r.at[l, c], device_id=dev, device_id_type=MESH)
            for i, dev, d_me in back_targets()
        ]

    def back_wait(l, c):
        wait_bytes(y1.at[l, pl.ds(0, others), cols_at(c)], c_r.at[l, c])

    home = 2 * n_line * cap

    def home_copy(l, c, m):
        s = mod(k_self + m)
        return pltpu.make_async_remote_copy(
            sendb.at[l, rows_at(s * home, home, 8), cols_at(c)], y3.at[l, rows_at(k_self * home, home, 8), cols_at(c)],
            e_s.at[0], e_r.at[l, c], device_id=mate(m), device_id_type=MESH)

    inputs = [
        pltpu.make_async_copy(src, dst, in_sem.at[n])
        for n, (src, dst) in enumerate(((idx_hbm, idx_ref), (x_hbm, x_ref), (gate_hbm, gate_ref)))
    ]
    for copy in inputs:
        copy.start()

    barrier = pltpu.get_barrier_semaphore()
    for side in (0, 1):
        for m in range(n_line):
            for dc in (0, 1):
                if (m, dc) == (0, 0) or (side and m == 0):
                    continue
                pos = mod((yy if side else xx) + m)
                c2 = lax.rem(cc + dc, 2)
                dev = (dp, pos, xx * 2 + c2) if side else (dp, yy, pos * 2 + c2)
                pl.semaphore_signal(barrier, inc=1, device_id=dev, device_id_type=MESH)

    for l in range(n_loc):
        for which in range(2):
            w13_copy(which, l).start()
    for t in range(n_w2):
        w2_copy(t).start()

    row_e = lax.broadcasted_iota(jnp.int32, (n_exp, n_tok), 0)
    inputs[0].wait()
    chosen = jnp.zeros((n_exp, n_tok), F32)
    for j in range(n_top):
        chosen = chosen + (idx_ref[j:j + 1, :] == row_e).astype(F32)
    before = (lax.broadcasted_iota(jnp.int32, (n_tok, n_tok), 0)
              < lax.broadcasted_iota(jnp.int32, (n_tok, n_tok), 1)).astype(BF16)
    slot = dot(chosen.astype(BF16), before)
    slot = jnp.where(chosen > 0, slot, -1.0).astype(BF16)
    mts[k_self] = slot

    with jax.named_scope('entry_wait'):
        pl.semaphore_wait(barrier, 4 * n_line - 3)

    inputs[1].wait()
    inputs[2].wait()
    for m in MATES:
        mt_copy(m).start()
    for h in range(ahead):
        for m in (1, 3):
            gather_copy(m, h).start()

    xg[rows_at(k_self * n_tok, n_tok, 8), :] = x_ref[...]

    r = lax.broadcasted_iota(jnp.int32, (n_rows, 1), 0)
    r12 = div12(r)
    r_slot = (r - r12 * cap).astype(F32)
    r_src = r12 & (n_line - 1)
    r_dev = r12 >> 2
    r_exp0 = coef_k * k_self + coef_q * (r_dev >> 1) + 2 * (r_dev & 1)
    e_lane = lax.broadcasted_iota(jnp.int32, (n_rows, n_exp), 1)
    with jax.named_scope('slots_wait'):
        wait_bytes(mts.at[pl.ds(0, n_line - 1)], mt_r.at[0])
    for l in range(n_loc):
        pick = (e_lane == r_exp0 + l).astype(BF16)
        for s in range(n_line):
            val = dot(pick, mts[s])
            hit = jnp.logical_and(val == r_slot, r_src == s)
            sel[l, :, s * n_tok:(s + 1) * n_tok] = jnp.where(hit, 1.0, 0.0).astype(BF16)

    def spread(l, h):
        sendb[l, :, half_cols(h)] = dot(sel[l], xg[:, half_cols(h)]).astype(BF16)
        for m, dc in PEERS:
            spread_copy(l, h, m, dc).start()
        rows[l, rows_at(i_self * per, per, 8), half_cols(h)] = sendb[l, rows_at(d_self * per, per, 8), half_cols(h)]

    def relay(h):
        for m in (1, 3):
            gather_copy(m, h).wait_recv()
            relay_copy(m, h).start()

    with jax.named_scope('gather_and_spread'):
        for h in range(lead):
            relay(h)
        for h in range(n_half):
            with jax.named_scope('gather_wait'):
                if h + lead < n_half:
                    relay(h + lead)
                if h + ahead < n_half:
                    for m in (1, 3):
                        gather_copy(m, h + ahead).start()
                for m in (1, 3):
                    relay_copy(m, h).wait_recv()
            with jax.named_scope('spread_send'):
                spread(0, h)
    with jax.named_scope('spread_rest'):
        for h in range(n_half):
            for l in range(1, n_loc):
                spread(l, h)

    o12 = r12
    o_in = (o12 & 7) * per + (o12 >> 3) * cap + (r - r12 * cap)
    perm[...] = (lax.broadcasted_iota(jnp.int32, (n_rows, n_rows), 1) == o_in).astype(BF16)

    gate = jnp.zeros((n_exp, n_tok), F32)
    for j in range(n_top):
        gate = gate + jnp.where(idx_ref[j:j + 1, :] == row_e, gate_ref[j:j + 1, :], 0.0)
    eye = (lax.broadcasted_iota(jnp.int32, (n_tok, n_tok), 0)
           == lax.broadcasted_iota(jnp.int32, (n_tok, n_tok), 1)).astype(BF16)
    slot_t = nt_dot(eye, mts[k_self]).astype(BF16)
    parts = []
    rest = gate
    for _ in range(3):
        part = rest.astype(BF16)
        parts.append(nt_dot(eye, part).astype(BF16))
        rest = rest - part.astype(F32)
    q = lax.broadcasted_iota(jnp.int32, (1, n_rows), 1)
    q12 = div12(q)
    q_slot = (q - q12 * cap).astype(F32)
    q_dev = q12 & 7
    q_exp0 = coef_k * (q12 >> 3) + coef_q * (q_dev >> 1) + 2 * (q_dev & 1)
    e_row = lax.broadcasted_iota(jnp.int32, (n_exp, n_rows), 0)
    for l in range(n_loc):
        spread_e = (e_row == q_exp0 + l).astype(BF16)
        hit = dot(slot_t, spread_e) == q_slot
        for p in range(3):
            gmat[l, p * n_tok:(p + 1) * n_tok, :] = jnp.where(hit, dot(parts[p], spread_e), 0.0).astype(BF16)
    acc[...] = x_ref[...].astype(F32)

    def expert_up(l, cuts):
        with jax.named_scope('weight_wait'):
            for which in range(2):
                w13_copy(which, l).wait()
        edges = (0,) + cuts + (n_half,)
        for h0, h1 in zip(edges, edges[1:]):
            with jax.named_scope('spread_wait'):
                for h in range(h0, h1):
                    spread_wait(l, h)
            k = slice(h0 * half, h1 * half)

            def tile(n, carry, h0=h0, h1=h1, k=k):
                cols = pl.ds(pl.multiple_of(n * f_tile, f_tile), f_tile)
                a = dot(rows[l, :, k], w1[l, k, cols])
                b = dot(rows[l, :, k], w3[l, k, cols])
                if h0 > 0:
                    a = a + part_a[:, cols]
                    b = b + part_b[:, cols]
                if h1 < n_half:
                    part_a[:, cols] = a
                    part_b[:, cols] = b
                else:
                    hid[:, cols] = (jax.nn.silu(a) * b).astype(BF16)
                return carry

            with jax.named_scope('up'):
                lax.fori_loop(0, ffn // f_tile, tile, 0)

    def expert_down(l, c):
        t = l * n_chunk + c
        w2_copy(t).wait()
        rows[l, :, cols_at(c)] = dot(hid[...], w2[lax.rem(t, n_w2)]).astype(BF16)

        @pl.when(t + n_w2 < n_loc * n_chunk)
        def _():
            w2_copy(t + n_w2).start()

        for copy in back_copies(l, c):
            copy.start()
        y1[l, rows_at(d_self * per, per, 8), cols_at(c)] = rows[l, rows_at(i_self * per, per, 8), cols_at(c)]

    def forward(l, c):
        with jax.named_scope('back_wait'):
            back_wait(l, c)
        sendb[l, :, cols_at(c)] = dot(perm[...], y1[l, :, cols_at(c)]).astype(BF16)
        for m in MATES:
            home_copy(l, c, m).start()
        y3[l, rows_at(k_self * home, home, 8), cols_at(c)] = sendb[l, rows_at(k_self * home, home, 8), cols_at(c)]

    def collect(l, c):
        with jax.named_scope('home_wait'):
            wait_bytes(y3.at[l, pl.ds(0, (n_line - 1) * home), cols_at(c)], e_r.at[l, c])
        part = dot(gmat[l], y3[l, :, cols_at(c)])
        acc[:, cols_at(c)] += part[:n_tok] + part[n_tok:2 * n_tok] + part[2 * n_tok:]

    def loop(body):
        def step(c, carry):
            body(c)
            return carry
        lax.fori_loop(0, n_chunk, step, 0)

    expert_up(0, cuts[0])
    with jax.named_scope('down0'):
        loop(lambda c: expert_down(0, c))
    expert_up(1, cuts[1])
    with jax.named_scope('spread_drain'):
        wait_bytes(sendb.at[:, pl.ds(0, others), :], d_s.at[0])

    def down_and_forward(c):
        expert_down(1, c)
        forward(0, c)

    with jax.named_scope('down1_forward0'):
        loop(down_and_forward)

    def forward_and_collect(c):
        forward(1, c)
        collect(0, c)

    with jax.named_scope('forward1_collect0'):
        loop(forward_and_collect)

    def finish(c):
        collect(1, c)
        out_ref[:, cols_at(c)] = acc[:, cols_at(c)].astype(BF16)

    with jax.named_scope('collect1'):
        loop(finish)

    with jax.named_scope('drain'):
        wait_bytes(mts.at[pl.ds(0, n_line - 1)], mt_s.at[0])
        wait_bytes(xg.at[pl.ds(0, (n_line - 1) * n_tok), :], g_s.at[0])
        wait_bytes(y1.at[:, pl.ds(0, others), :], c_s.at[0])
        wait_bytes(y3.at[:, pl.ds(0, (n_line - 1) * home), :], e_s.at[0])


def solution(mesh):
    group_axes = ('ep2', 'ep')
    n_line = mesh.shape['ep2']
    n_group = n_line * mesh.shape['ep']
    row_spec = P(('dp', 'ep2', 'ep'), None)
    weight_spec = P(group_axes, None, None)

    def device_step(tokens, expert_ids, gates, w_gate, w_up, w_down):
        n_tok, n_top = expert_ids.shape
        n_loc, dim, ffn = w_gate.shape
        n_exp = n_loc * n_group
        cap = -(-(n_tok * n_top) // n_exp)
        n_rows = n_group * cap
        n_half, n_chunk, f_tile, n_w2, cuts, ahead, lead = 5, 5, 256, 3, ((2, 4), (2, 4)), 5, 5
        sem = pltpu.SemaphoreType.DMA
        vmem = pl.BlockSpec(memory_space=pltpu.VMEM)
        hbm = pl.BlockSpec(memory_space=pl.ANY)
        n_dev = 2 * n_line
        return pl.pallas_call(
            functools.partial(moe_kernel, n_line, cap, n_half, n_chunk, f_tile, cuts, ahead, lead),
            out_shape=jax.ShapeDtypeStruct((n_tok, dim), BF16),
            in_specs=[hbm] * 6,
            out_specs=vmem,
            scratch_shapes=[
                pltpu.VMEM((n_tok, dim), BF16),
                pltpu.VMEM((n_top, n_tok), jnp.int32),
                pltpu.VMEM((n_top, n_tok), F32),
                pltpu.VMEM((n_loc, dim, ffn), BF16),
                pltpu.VMEM((n_loc, dim, ffn), BF16),
                pltpu.VMEM((n_w2, ffn, dim // n_chunk), BF16),
                pltpu.VMEM((n_line, n_exp, n_tok), BF16),
                pltpu.VMEM((n_line * n_tok, dim), BF16),
                pltpu.VMEM((n_loc, n_rows, n_line * n_tok), BF16),
                pltpu.VMEM((n_loc, n_rows, dim), BF16),
                pltpu.VMEM((n_loc, n_rows, dim), BF16),
                pltpu.VMEM((n_rows, ffn), F32),
                pltpu.VMEM((n_rows, ffn), F32),
                pltpu.VMEM((n_rows, ffn), BF16),
                pltpu.VMEM((n_loc, n_rows, dim), BF16),
                pltpu.VMEM((n_loc, n_rows, dim), BF16),
                pltpu.VMEM((n_rows, n_rows), BF16),
                pltpu.VMEM((n_loc, 3 * n_tok, n_rows), BF16),
                pltpu.VMEM((n_tok, dim), F32),
                sem((3,)),
                sem((2, n_loc)),
                sem((n_w2,)),
                sem((1,)), sem((1,)),
                sem((1,)), sem((4, n_half)),
                sem((1,)), sem((n_loc, n_half)),
                sem((1,)), sem((n_loc, n_chunk)),
                sem((1,)), sem((n_loc, n_chunk)),
            ],
            compiler_params=pltpu.CompilerParams(
                collective_id=0, has_side_effects=True, vmem_limit_bytes=67043328),
        )(tokens, expert_ids.T, gates.T, w_gate, w_up, w_down)

    return jax.shard_map(
        device_step, mesh=mesh,
        in_specs=(row_spec, row_spec, row_spec, weight_spec, weight_spec, weight_spec),
        out_specs=row_spec, check_vma=False)
```

```python
import functools

import jax
import jax.numpy as jnp
from jax import lax
from jax.experimental import pallas as pl
from jax.experimental.pallas import tpu as pltpu
from jax.sharding import PartitionSpec as P

MESH = pl.DeviceIdType.MESH
F32 = jnp.float32
BF16 = jnp.bfloat16
PEERS = [(1, 0), (3, 0), (1, 1), (3, 1), (2, 0), (2, 1), (0, 1)]
MATES = [1, 3, 2]


def div12(v):
    return (v * 2731) >> 15


def nt_dot(a, b):
    return lax.dot_general(a, b, (((1,), (1,)), ((), ())), preferred_element_type=F32)


def dot(a, b):
    return jnp.dot(a, b, preferred_element_type=F32)


def moe_kernel(
    n_line, cap, n_half, n_chunk, f_tile, cuts, ahead, lag,
    x_hbm, idx_hbm, gate_hbm, w1_hbm, w3_hbm, w2_hbm, out_hbm,
    x_ref, idx_ref, gate_ref, w1, w3, w2, slots, gates, mts, slots_far, gates_near, xg, sel, sendb, rows, part_a, part_b, hid, y1,
    y_raw, y_far, perm, gmat, acc, part_out, part_in,
    in_sem, out_sem, w13_sem, w2_sem, mt_s, mt_r, n_s, n_r, g_s, g_r, d_s, d_r, c_s, c_r, e_s, e_r, f_r, p_s, p_r,
):
    n_tok, dim = x_ref.shape
    n_top = idx_ref.shape[0]
    n_loc, ffn = w2_hbm.shape[0], w2_hbm.shape[1]
    n_exp = slots.shape[0]
    n_line_exp = n_exp // n_line
    per = n_line * cap
    n_rows = 2 * n_line * per
    n_w2 = w2.shape[0]
    half = dim // n_half
    wide = dim // n_chunk

    dp = lax.axis_index('dp')
    yy = lax.axis_index('ep2')
    ee = lax.axis_index('ep')
    xx = ee // 2
    cc = lax.rem(ee, 2)
    k_self = jnp.where(cc == 0, yy, xx)
    q_self = jnp.where(cc == 0, xx, yy)
    i_self = cc * n_line + q_self
    d_self = 2 * q_self + cc
    coef_k = jnp.where(cc == 0, 16, 4)
    coef_q = jnp.where(cc == 0, 4, 16)

    def mod(v):
        return lax.rem(v + n_line, n_line)

    def mate(m):
        k = mod(k_self + m)
        return (dp, jnp.where(cc == 0, k, yy), jnp.where(cc == 0, xx, k) * 2 + cc)

    def spread_peer(m, dc):
        q = mod(q_self + m)
        c2 = lax.rem(cc + dc, 2)
        dev = (dp, jnp.where(cc == 0, yy, q), jnp.where(cc == 0, q, xx) * 2 + c2)
        return dev, 2 * q + c2

    def rows_at(start, size, unit):
        return pl.ds(pl.multiple_of(start, unit), size)

    def half_cols(h):
        return pl.ds(h * half, half)

    def cols_at(c):
        return pl.ds(pl.multiple_of(c * wide, wide), wide)

    def w13_copy(which, l):
        hbm, buf = ((w1_hbm, w1), (w3_hbm, w3))[which]
        return pltpu.make_async_copy(hbm.at[l], buf.at[l], w13_sem.at[which, l])

    def w2_copy(t):
        slot = lax.rem(t, n_w2)
        return pltpu.make_async_copy(
            w2_hbm.at[t // n_chunk, :, cols_at(lax.rem(t, n_chunk))], w2.at[slot], w2_sem.at[slot])

    def mt_copy(m):
        return pltpu.make_async_remote_copy(
            slots.at[line_rows(mod(k_self + m)), :], mts.at[k_self], mt_s.at[0], mt_r.at[0], device_id=mate(m), device_id_type=MESH)

    def gather_copy(m, h):
        return pltpu.make_async_remote_copy(
            x_ref.at[:, half_cols(h)], xg.at[rows_at(k_self * n_tok, n_tok, 8), half_cols(h)],
            g_s.at[0], g_r.at[m // 2, h], device_id=mate(m), device_id_type=MESH)

    def relay_copy(m, h):
        side = m // 2
        block = xg.at[rows_at(mod(k_self - m) * n_tok + side * (n_tok // 2), n_tok // 2, 8), half_cols(h)]
        return pltpu.make_async_remote_copy(
            block, block, g_s.at[0], g_r.at[2 + side, h], device_id=mate(m), device_id_type=MESH)

    def wait_bytes(ref, sem):
        pltpu.make_async_copy(ref, ref, sem).wait()

    def spread_copy(l, h, m, dc):
        dev, d = spread_peer(m, dc)
        return pltpu.make_async_remote_copy(
            sendb.at[l, rows_at(d * per, per, 8), half_cols(h)],
            rows.at[l, rows_at(i_self * per, per, 8), half_cols(h)],
            d_s.at[0], d_r.at[l, h], device_id=dev, device_id_type=MESH)

    others = (2 * n_line - 1) * per

    def spread_wait(l, h):
        wait_bytes(rows.at[l, pl.ds(0, others), half_cols(h)], d_r.at[l, h])

    def back_targets():
        out = []
        for m in (1, 3, 2):
            for side in (0, 1):
                pos = mod((yy if side else xx) + m)
                dev = (dp, pos, xx * 2 + 1) if side else (dp, yy, pos * 2)
                d_me = 2 * (yy if side else xx) + cc
                out.append((side * n_line + pos, dev, d_me))
        other = 1 - cc
        pos = jnp.where(other == 0, xx, yy)
        out.append((other * n_line + pos, (dp, yy, xx * 2 + other), 2 * pos + cc))
        return out

    def back_copies(l, c):
        return [
            pltpu.make_async_remote_copy(
                rows.at[l, rows_at(i * per, per, 8), cols_at(c)], y1.at[l, rows_at(d_me * per, per, 8), cols_at(c)],
                c_s.at[0], c_r.at[l, c], device_id=dev, device_id_type=MESH)
            for i, dev, d_me in back_targets()
        ]

    def back_wait(l, c):
        wait_bytes(y1.at[l, pl.ds(0, others), cols_at(c)], c_r.at[l, c])

    home = 2 * n_line * cap
    both = n_loc * home

    def at_home(s, l):
        return s >> 1, rows_at((s & 1) * both + l * home, home, 8)

    def side_cols(c, side):
        return pl.ds(pl.multiple_of(c * wide + side * (wide // 2), wide // 2), wide // 2)

    def raw_copy(l, c, m):
        side = m // 2
        p, r = at_home(mod(k_self + m), l)
        return pltpu.make_async_remote_copy(
            sendb.at[p, r, side_cols(c, side)], y_raw.at[pl.ds(l * home, home), side_cols(c, side)],
            e_s.at[0], e_r.at[c], device_id=mate(m), device_id_type=MESH)

    def far_copy(l, c, m):
        side = 1 - m // 2
        p, r = at_home(mod(k_self + 2), l)
        return pltpu.make_async_remote_copy(
            sendb.at[p, r, side_cols(c, side)], y_far.at[pl.ds(l * home, home), side_cols(c, side)],
            e_s.at[0], f_r.at[c], device_id=mate(m), device_id_type=MESH)

    def sum_copy(c, m):
        cols = side_cols(c, 1 - m // 2)
        return pltpu.make_async_remote_copy(
            part_out.at[:, cols], part_in.at[:, cols], p_s.at[0], p_r.at[c], device_id=mate(m), device_id_type=MESH)

    def line_rows(k):
        return pl.ds(pl.multiple_of(k * n_line_exp, n_line_exp), n_line_exp)

    def note_copies(m):
        side = m // 2
        out = [pltpu.make_async_remote_copy(
            slots.at[line_rows(mod(k_self + 2)), :], slots_far.at[side], n_s.at[0], n_r.at[0],
            device_id=mate(m), device_id_type=MESH)]
        for n, k in enumerate((mod(k_self + m), mod(k_self + 2))):
            out.append(pltpu.make_async_remote_copy(
                gates.at[line_rows(k), :], gates_near.at[side, n], n_s.at[1], n_r.at[1],
                device_id=mate(m), device_id_type=MESH))
        return out

    inputs = [
        pltpu.make_async_copy(src, dst, in_sem.at[n])
        for n, (src, dst) in enumerate(((idx_hbm, idx_ref), (x_hbm, x_ref), (gate_hbm, gate_ref)))
    ]
    for copy in inputs:
        copy.start()

    barrier = pltpu.get_barrier_semaphore()
    for side in (0, 1):
        for m in range(n_line):
            for dc in (0, 1):
                if (m, dc) == (0, 0) or (side and m == 0):
                    continue
                pos = mod((yy if side else xx) + m)
                c2 = lax.rem(cc + dc, 2)
                dev = (dp, pos, xx * 2 + c2) if side else (dp, yy, pos * 2 + c2)
                pl.semaphore_signal(barrier, inc=1, device_id=dev, device_id_type=MESH)

    for l in range(n_loc):
        for which in range(2):
            w13_copy(which, l).start()
    for t in range(n_w2):
        w2_copy(t).start()

    r_e = lax.broadcasted_iota(jnp.int32, (n_exp, n_tok), 0)
    row_e = (coef_k * (r_e >> 4) + coef_q * ((r_e >> 2) & 3) + (r_e & 3))
    inputs[0].wait()
    chosen = jnp.zeros((n_exp, n_tok), F32)
    for j in range(n_top):
        chosen = chosen + (idx_ref[j:j + 1, :] == row_e).astype(F32)
    before = (lax.broadcasted_iota(jnp.int32, (n_tok, n_tok), 0)
              < lax.broadcasted_iota(jnp.int32, (n_tok, n_tok), 1)).astype(BF16)
    slot = dot(chosen.astype(BF16), before)
    slot = jnp.where(chosen > 0, slot, -1.0).astype(BF16)
    slots[...] = slot
    mts[k_self] = slots[line_rows(k_self), :]

    inputs[2].wait()
    gate = jnp.zeros((n_exp, n_tok), F32)
    for j in range(n_top):
        gate = gate + jnp.where(idx_ref[j:j + 1, :] == row_e, gate_ref[j:j + 1, :], 0.0)
    gates[...] = gate

    with jax.named_scope('entry_wait'):
        pl.semaphore_wait(barrier, 4 * n_line - 3)

    inputs[1].wait()
    for m in MATES:
        mt_copy(m).start()
    for h in range(ahead):
        for m in (1, 3):
            gather_copy(m, h).start()

    xg[rows_at(k_self * n_tok, n_tok, 8), :] = x_ref[...]

    r = lax.broadcasted_iota(jnp.int32, (n_rows, 1), 0)
    r12 = div12(r)
    r_slot = (r - r12 * cap).astype(F32)
    r_src = r12 & (n_line - 1)
    r_dev = r12 >> 2
    e_lane = lax.broadcasted_iota(jnp.int32, (n_rows, n_line_exp), 1)
    with jax.named_scope('slots_wait'):
        wait_bytes(mts.at[pl.ds(0, n_line - 1)], mt_r.at[0])
    for l in range(n_loc):
        pick = (e_lane == n_loc * r_dev + l).astype(BF16)
        for s in range(n_line):
            val = dot(pick, mts[s])
            hit = jnp.logical_and(val == r_slot, r_src == s)
            sel[l, :, s * n_tok:(s + 1) * n_tok] = jnp.where(hit, 1.0, 0.0).astype(BF16)

    def spread(l, h):
        sendb[l, :, half_cols(h)] = dot(sel[l], xg[:, half_cols(h)]).astype(BF16)
        for m, dc in PEERS:
            spread_copy(l, h, m, dc).start()
        rows[l, rows_at(i_self * per, per, 8), half_cols(h)] = sendb[l, rows_at(d_self * per, per, 8), half_cols(h)]

    def relay(h):
        for m in (1, 3):
            gather_copy(m, h).wait_recv()
            relay_copy(m, h).start()

    with jax.named_scope('gather_and_spread'):
        for h in range(n_half):
            relay(h)
            if h + ahead < n_half:
                for m in (1, 3):
                    gather_copy(m, h + ahead).start()
        for m in (1, 3):
            for copy in note_copies(m):
                copy.start()
        for h in range(n_half):
            with jax.named_scope('gather_wait'):
                for m in (1, 3):
                    relay_copy(m, h).wait_recv()
            with jax.named_scope('spread_send'):
                spread(0, h)
    with jax.named_scope('spread_rest'):
        for h in range(n_half):
            for l in range(1, n_loc):
                spread(l, h)

    o12 = r12
    o_in = (o12 & 7) * per + (o12 >> 3) * cap + (r - r12 * cap)
    perm[...] = (lax.broadcasted_iota(jnp.int32, (n_rows, n_rows), 1) == o_in).astype(BF16)

    eye = (lax.broadcasted_iota(jnp.int32, (n_tok, n_tok), 0)
           == lax.broadcasted_iota(jnp.int32, (n_tok, n_tok), 1)).astype(BF16)
    q = lax.broadcasted_iota(jnp.int32, (1, both), 1)
    q12 = div12(q)
    q_slot = (q - q12 * cap).astype(F32)
    q_exp = n_loc * (q12 & 7) + (q12 >> 3)
    spread_e = (lax.broadcasted_iota(jnp.int32, (n_line_exp, both), 0) == q_exp).astype(BF16)

    def gate_block(slot_rows, gate_rows, put):
        hit = dot(nt_dot(eye, slot_rows).astype(BF16), spread_e) == q_slot
        rest = gate_rows
        for p in range(3):
            part = rest.astype(BF16)
            rest = rest - part.astype(F32)
            put(p, jnp.where(hit, dot(nt_dot(eye, part).astype(BF16), spread_e), 0.0).astype(BF16))

    for n, m in enumerate((0, 3, 1)):
        k = line_rows(mod(k_self + m))

        def put_own(p, v, n=n):
            gmat[n, p * n_tok:(p + 1) * n_tok, :] = v

        gate_block(slots[k, :], gates[k, :], put_own)
    wait_bytes(slots_far, n_r.at[0])
    wait_bytes(gates_near, n_r.at[1])
    for side in range(2):
        for n in range(2):
            near = mts[mod(k_self + (3 if side == 0 else 1))] if n == 0 else slots_far[side]

            def put_near(p, v, side=side, n=n):
                sel[side, p * n_tok:(p + 1) * n_tok, n * 256:n * 256 + both] = v

            gate_block(near, gates_near[side, n], put_near)
    acc[...] = x_ref[...].astype(F32)

    def expert_up(l, cuts):
        with jax.named_scope('weight_wait'):
            for which in range(2):
                w13_copy(which, l).wait()
        edges = (0,) + cuts + (n_half,)
        for h0, h1 in zip(edges, edges[1:]):
            with jax.named_scope('spread_wait'):
                for h in range(h0, h1):
                    spread_wait(l, h)
            k = slice(h0 * half, h1 * half)

            def tile(n, carry, h0=h0, h1=h1, k=k):
                cols = pl.ds(pl.multiple_of(n * f_tile, f_tile), f_tile)
                a = dot(rows[l, :, k], w1[l, k, cols])
                b = dot(rows[l, :, k], w3[l, k, cols])
                if h0 > 0:
                    a = a + part_a[:, cols]
                    b = b + part_b[:, cols]
                if h1 < n_half:
                    part_a[:, cols] = a
                    part_b[:, cols] = b
                else:
                    hid[:, cols] = (jax.nn.silu(a) * b).astype(BF16)
                return carry

            with jax.named_scope('up'):
                lax.fori_loop(0, ffn // f_tile, tile, 0)

    def expert_down(l, c):
        t = l * n_chunk + c
        w2_copy(t).wait()
        rows[l, :, cols_at(c)] = dot(hid[...], w2[lax.rem(t, n_w2)]).astype(BF16)

        @pl.when(t + n_w2 < n_loc * n_chunk)
        def _():
            w2_copy(t + n_w2).start()

        for copy in back_copies(l, c):
            copy.start()
        y1[l, rows_at(d_self * per, per, 8), cols_at(c)] = rows[l, rows_at(i_self * per, per, 8), cols_at(c)]

    def forward(l, c):
        with jax.named_scope('back_wait'):
            back_wait(l, c)
        out = dot(perm[...], y1[l, :, cols_at(c)]).astype(BF16)
        for s in range(n_line):
            sendb[s >> 1, (s & 1) * both + l * home:(s & 1) * both + (l + 1) * home, cols_at(c)] = (
                out[s * home:(s + 1) * home])
        for m in (1, 3):
            far_copy(l, c, m).start()
        for m in (1, 3):
            raw_copy(l, c, m).start()

    def fold(v):
        return v[:n_tok] + v[n_tok:2 * n_tok] + v[2 * n_tok:]

    def home_rows(s):
        return s >> 1, rows_at((s & 1) * both, both, 8)

    def own_sums(c):
        p, r = home_rows(k_self)
        acc[:, cols_at(c)] += fold(dot(gmat[0], sendb[p, r, cols_at(c)]))
        for side, m in ((0, 3), (1, 1)):
            p, r = home_rows(mod(k_self + m))
            part_out[:, side_cols(c, side)] = fold(
                dot(sel[side, :, 0:both], sendb[p, r, side_cols(c, side)]))

    def merge(c):
        with jax.named_scope('far_wait'):
            wait_bytes(y_far.at[:, cols_at(c)], f_r.at[c])
        for side in range(2):
            cols = side_cols(c, side)
            part_out[:, cols] += fold(dot(sel[side, :, 256:256 + both], y_far[:, cols]))
        for m in (1, 3):
            sum_copy(c, m).start()

    def collect(c):
        with jax.named_scope('raw_wait'):
            wait_bytes(y_raw.at[:, cols_at(c)], e_r.at[c])
        for side in range(2):
            cols = side_cols(c, side)
            acc[:, cols] += fold(dot(gmat[1 + side], y_raw[:, cols]))

    def loop(body, start=0, stop=n_chunk):
        def step(c, carry):
            body(c)
            return carry
        lax.fori_loop(start, stop, step, 0)

    expert_up(0, cuts[0])
    with jax.named_scope('down0'):
        loop(lambda c: expert_down(0, c))
    expert_up(1, cuts[1])
    with jax.named_scope('spread_drain'):
        wait_bytes(sendb.at[:, pl.ds(0, others), :], d_s.at[0])

    def down_and_forward(c):
        expert_down(1, c)
        forward(0, c)

    with jax.named_scope('down1_forward0'):
        loop(down_and_forward)

    def forward_and_sum(c):
        forward(1, c)
        own_sums(c)

    def forward_and_merge(c):
        forward_and_sum(c)
        merge(c - lag)

    with jax.named_scope('forward1'):
        loop(forward_and_sum, 0, lag)
        loop(forward_and_merge, lag, n_chunk)

    def merge_and_collect(c):
        merge(c)
        collect(c - n_chunk + lag)

    with jax.named_scope('merge'):
        loop(merge_and_collect, n_chunk - lag, n_chunk)
        loop(collect, lag, n_chunk)
    wait_bytes(xg.at[pl.ds(0, (n_line - 1) * n_tok), :], g_s.at[0])

    def finish(c):
        with jax.named_scope('sum_wait'):
            wait_bytes(part_in.at[:, cols_at(c)], p_r.at[c])
        x_ref[:, cols_at(c)] = (acc[:, cols_at(c)] + part_in[:, cols_at(c)]).astype(BF16)
        pltpu.make_async_copy(x_ref.at[:, cols_at(c)], out_hbm.at[:, cols_at(c)], out_sem.at[0]).start()

    with jax.named_scope('finish'):
        loop(finish)

    with jax.named_scope('drain'):
        wait_bytes(x_ref, out_sem.at[0])
        wait_bytes(mts.at[pl.ds(0, n_line - 1)], mt_s.at[0])
        wait_bytes(slots_far, n_s.at[0])
        wait_bytes(gates_near, n_s.at[1])
        wait_bytes(y1.at[:, pl.ds(0, others), :], c_s.at[0])
        wait_bytes(y1.at[0], e_s.at[0])
        wait_bytes(part_out, p_s.at[0])


def solution(mesh):
    group_axes = ('ep2', 'ep')
    n_line = mesh.shape['ep2']
    n_group = n_line * mesh.shape['ep']
    row_spec = P(('dp', 'ep2', 'ep'), None)
    weight_spec = P(group_axes, None, None)

    def device_step(tokens, expert_ids, gates, w_gate, w_up, w_down):
        n_tok, n_top = expert_ids.shape
        n_loc, dim, ffn = w_gate.shape
        n_exp = n_loc * n_group
        cap = -(-(n_tok * n_top) // n_exp)
        n_rows = n_group * cap
        n_half, n_chunk, f_tile, n_w2, cuts, ahead, lag = 5, 5, 256, 3, ((2, 4), (2, 4)), 5, 3
        sem = pltpu.SemaphoreType.DMA
        hbm = pl.BlockSpec(memory_space=pl.ANY)
        n_dev = 2 * n_line
        return pl.pallas_call(
            functools.partial(moe_kernel, n_line, cap, n_half, n_chunk, f_tile, cuts, ahead, lag),
            out_shape=jax.ShapeDtypeStruct((n_tok, dim), BF16),
            in_specs=[hbm] * 6,
            out_specs=hbm,
            scratch_shapes=[
                pltpu.VMEM((n_tok, dim), BF16),
                pltpu.VMEM((n_top, n_tok), jnp.int32),
                pltpu.VMEM((n_top, n_tok), F32),
                pltpu.VMEM((n_loc, dim, ffn), BF16),
                pltpu.VMEM((n_loc, dim, ffn), BF16),
                pltpu.VMEM((n_w2, ffn, dim // n_chunk), BF16),
                pltpu.VMEM((n_exp, n_tok), BF16),
                pltpu.VMEM((n_exp, n_tok), F32),
                pltpu.VMEM((n_line, n_exp // n_line, n_tok), BF16),
                pltpu.VMEM((2, n_exp // n_line, n_tok), BF16),
                pltpu.VMEM((2, 2, n_exp // n_line, n_tok), F32),
                pltpu.VMEM((n_line * n_tok, dim), BF16),
                pltpu.VMEM((n_loc, n_rows, n_line * n_tok), BF16),
                pltpu.VMEM((n_loc, n_rows, dim), BF16),
                pltpu.VMEM((n_loc, n_rows, dim), BF16),
                pltpu.VMEM((n_rows, ffn), F32),
                pltpu.VMEM((n_rows, ffn), F32),
                pltpu.VMEM((n_rows, ffn), BF16),
                pltpu.VMEM((n_loc, n_rows, dim), BF16),
                pltpu.VMEM((n_loc * n_dev * cap, dim), BF16),
                pltpu.VMEM((n_loc * n_dev * cap, dim), BF16),
                pltpu.VMEM((n_rows, n_rows), BF16),
                pltpu.VMEM((3, 3 * n_tok, n_loc * n_dev * cap), BF16),
                pltpu.VMEM((n_tok, dim), F32),
                pltpu.VMEM((n_tok, dim), F32),
                pltpu.VMEM((n_tok, dim), F32),
                sem((3,)),
                sem((1,)),
                sem((2, n_loc)),
                sem((n_w2,)),
                sem((1,)), sem((1,)),
                sem((2,)), sem((2,)),
                sem((1,)), sem((4, n_half)),
                sem((1,)), sem((n_loc, n_half)),
                sem((1,)), sem((n_loc, n_chunk)),
                sem((1,)), sem((n_chunk,)), sem((n_chunk,)),
                sem((1,)), sem((n_chunk,)),
            ],
            compiler_params=pltpu.CompilerParams(
                collective_id=0, has_side_effects=True, vmem_limit_bytes=67043328),
        )(tokens, expert_ids.T, gates.T, w_gate, w_up, w_down)

    return jax.shard_map(
        device_step, mesh=mesh,
        in_specs=(row_spec, row_spec, row_spec, weight_spec, weight_spec, weight_spec),
        out_specs=row_spec, check_vma=False)
```

```python
import functools

import jax
import jax.numpy as jnp
from jax import lax
from jax.experimental import pallas as pl
from jax.experimental.pallas import tpu as pltpu
from jax.sharding import PartitionSpec as P

MESH = pl.DeviceIdType.MESH
F32 = jnp.float32
BF16 = jnp.bfloat16
PEERS = [(1, 0), (3, 0), (1, 1), (3, 1), (2, 0), (2, 1), (0, 1)]
MATES = [1, 3, 2]


def div12(v):
    return (v * 2731) >> 15


def nt_dot(a, b):
    return lax.dot_general(a, b, (((1,), (1,)), ((), ())), preferred_element_type=F32)


def dot(a, b):
    return jnp.dot(a, b, preferred_element_type=F32)


def moe_kernel(
    n_line, cap, n_half, n_chunk, f_tile, cuts, ahead, lead, lag,
    x_hbm, idx_hbm, gate_hbm, w1_hbm, w3_hbm, w2_hbm, out_ref,
    x_ref, idx_ref, gate_ref, w1, w3, w2, slots, gates, mts, slots_far, gates_near, xg, sel, sendb, rows, part_a, part_b, hid, y1,
    y_raw, y_far, perm, gmat, acc, part_out, part_in,
    in_sem, w13_sem, w2_sem, mt_s, mt_r, n_s, n_r, g_s, g_r, d_s, d_r, c_s, c_r, e_s, e_r, f_r, p_s, p_r,
):
    n_tok, dim = x_ref.shape
    n_top = idx_ref.shape[0]
    n_loc, ffn = w2_hbm.shape[0], w2_hbm.shape[1]
    n_exp = slots.shape[0]
    n_line_exp = n_exp // n_line
    per = n_line * cap
    n_rows = 2 * n_line * per
    n_w2 = w2.shape[0]
    half = dim // n_half
    wide = dim // n_chunk

    dp = lax.axis_index('dp')
    yy = lax.axis_index('ep2')
    ee = lax.axis_index('ep')
    xx = ee // 2
    cc = lax.rem(ee, 2)
    k_self = jnp.where(cc == 0, yy, xx)
    q_self = jnp.where(cc == 0, xx, yy)
    i_self = cc * n_line + q_self
    d_self = 2 * q_self + cc
    coef_k = jnp.where(cc == 0, 16, 4)
    coef_q = jnp.where(cc == 0, 4, 16)

    def mod(v):
        return lax.rem(v + n_line, n_line)

    def mate(m):
        k = mod(k_self + m)
        return (dp, jnp.where(cc == 0, k, yy), jnp.where(cc == 0, xx, k) * 2 + cc)

    def spread_peer(m, dc):
        q = mod(q_self + m)
        c2 = lax.rem(cc + dc, 2)
        dev = (dp, jnp.where(cc == 0, yy, q), jnp.where(cc == 0, q, xx) * 2 + c2)
        return dev, 2 * q + c2

    def rows_at(start, size, unit):
        return pl.ds(pl.multiple_of(start, unit), size)

    def half_cols(h):
        return pl.ds(h * half, half)

    def cols_at(c):
        return pl.ds(pl.multiple_of(c * wide, wide), wide)

    def w13_copy(which, l):
        hbm, buf = ((w1_hbm, w1), (w3_hbm, w3))[which]
        return pltpu.make_async_copy(hbm.at[l], buf.at[l], w13_sem.at[which, l])

    def w2_copy(t):
        slot = lax.rem(t, n_w2)
        return pltpu.make_async_copy(
            w2_hbm.at[t // n_chunk, :, cols_at(lax.rem(t, n_chunk))], w2.at[slot], w2_sem.at[slot])

    def mt_copy(m):
        return pltpu.make_async_remote_copy(
            slots.at[line_rows(mod(k_self + m)), :], mts.at[k_self], mt_s.at[0], mt_r.at[0], device_id=mate(m), device_id_type=MESH)

    def gather_copy(m, h):
        return pltpu.make_async_remote_copy(
            x_ref.at[:, half_cols(h)], xg.at[rows_at(k_self * n_tok, n_tok, 8), half_cols(h)],
            g_s.at[0], g_r.at[m // 2, h], device_id=mate(m), device_id_type=MESH)

    def relay_copy(m, h):
        side = m // 2
        block = xg.at[rows_at(mod(k_self - m) * n_tok + side * (n_tok // 2), n_tok // 2, 8), half_cols(h)]
        return pltpu.make_async_remote_copy(
            block, block, g_s.at[0], g_r.at[2 + side, h], device_id=mate(m), device_id_type=MESH)

    def wait_bytes(ref, sem):
        pltpu.make_async_copy(ref, ref, sem).wait()

    def spread_copy(l, h, m, dc):
        dev, d = spread_peer(m, dc)
        return pltpu.make_async_remote_copy(
            sendb.at[l, rows_at(d * per, per, 8), half_cols(h)],
            rows.at[l, rows_at(i_self * per, per, 8), half_cols(h)],
            d_s.at[0], d_r.at[l, h], device_id=dev, device_id_type=MESH)

    others = (2 * n_line - 1) * per

    def spread_wait(l, h):
        wait_bytes(rows.at[l, pl.ds(0, others), half_cols(h)], d_r.at[l, h])

    def back_targets():
        out = []
        for m in (1, 3, 2):
            for side in (0, 1):
                pos = mod((yy if side else xx) + m)
                dev = (dp, pos, xx * 2 + 1) if side else (dp, yy, pos * 2)
                d_me = 2 * (yy if side else xx) + cc
                out.append((side * n_line + pos, dev, d_me))
        other = 1 - cc
        pos = jnp.where(other == 0, xx, yy)
        out.append((other * n_line + pos, (dp, yy, xx * 2 + other), 2 * pos + cc))
        return out

    def back_copies(l, c):
        return [
            pltpu.make_async_remote_copy(
                rows.at[l, rows_at(i * per, per, 8), cols_at(c)], y1.at[l, rows_at(d_me * per, per, 8), cols_at(c)],
                c_s.at[0], c_r.at[l, c], device_id=dev, device_id_type=MESH)
            for i, dev, d_me in back_targets()
        ]

    def back_wait(l, c):
        wait_bytes(y1.at[l, pl.ds(0, others), cols_at(c)], c_r.at[l, c])

    home = 2 * n_line * cap
    both = n_loc * home

    def at_home(s, l):
        return s >> 1, rows_at((s & 1) * both + l * home, home, 8)

    def side_cols(c, side):
        return pl.ds(pl.multiple_of(c * wide + side * (wide // 2), wide // 2), wide // 2)

    def raw_copy(l, c, m):
        side = m // 2
        p, r = at_home(mod(k_self + m), l)
        return pltpu.make_async_remote_copy(
            sendb.at[p, r, side_cols(c, side)], y_raw.at[pl.ds(l * home, home), side_cols(c, side)],
            e_s.at[0], e_r.at[c], device_id=mate(m), device_id_type=MESH)

    def far_copy(l, c, m):
        side = 1 - m // 2
        p, r = at_home(mod(k_self + 2), l)
        return pltpu.make_async_remote_copy(
            sendb.at[p, r, side_cols(c, side)], y_far.at[pl.ds(l * home, home), side_cols(c, side)],
            e_s.at[0], f_r.at[c], device_id=mate(m), device_id_type=MESH)

    def sum_copy(c, m):
        cols = side_cols(c, 1 - m // 2)
        return pltpu.make_async_remote_copy(
            part_out.at[:, cols], part_in.at[:, cols], p_s.at[0], p_r.at[c], device_id=mate(m), device_id_type=MESH)

    def line_rows(k):
        return pl.ds(pl.multiple_of(k * n_line_exp, n_line_exp), n_line_exp)

    def note_copies(m):
        side = m // 2
        out = [pltpu.make_async_remote_copy(
            slots.at[line_rows(mod(k_self + 2)), :], slots_far.at[side], n_s.at[0], n_r.at[0],
            device_id=mate(m), device_id_type=MESH)]
        for n, k in enumerate((mod(k_self + m), mod(k_self + 2))):
            out.append(pltpu.make_async_remote_copy(
                gates.at[line_rows(k), :], gates_near.at[side, n], n_s.at[1], n_r.at[1],
                device_id=mate(m), device_id_type=MESH))
        return out

    inputs = [
        pltpu.make_async_copy(src, dst, in_sem.at[n])
        for n, (src, dst) in enumerate(((idx_hbm, idx_ref), (x_hbm, x_ref), (gate_hbm, gate_ref)))
    ]
    for copy in inputs:
        copy.start()

    barrier = pltpu.get_barrier_semaphore()
    for side in (0, 1):
        for m in range(n_line):
            for dc in (0, 1):
                if (m, dc) == (0, 0) or (side and m == 0):
                    continue
                pos = mod((yy if side else xx) + m)
                c2 = lax.rem(cc + dc, 2)
                dev = (dp, pos, xx * 2 + c2) if side else (dp, yy, pos * 2 + c2)
                pl.semaphore_signal(barrier, inc=1, device_id=dev, device_id_type=MESH)

    for l in range(n_loc):
        for which in range(2):
            w13_copy(which, l).start()
    for t in range(n_w2):
        w2_copy(t).start()

    r_e = lax.broadcasted_iota(jnp.int32, (n_exp, n_tok), 0)
    row_e = (coef_k * (r_e >> 4) + coef_q * ((r_e >> 2) & 3) + (r_e & 3))
    inputs[0].wait()
    chosen = jnp.zeros((n_exp, n_tok), F32)
    for j in range(n_top):
        chosen = chosen + (idx_ref[j:j + 1, :] == row_e).astype(F32)
    before = (lax.broadcasted_iota(jnp.int32, (n_tok, n_tok), 0)
              < lax.broadcasted_iota(jnp.int32, (n_tok, n_tok), 1)).astype(BF16)
    slot = dot(chosen.astype(BF16), before)
    slot = jnp.where(chosen > 0, slot, -1.0).astype(BF16)
    slots[...] = slot
    mts[k_self] = slots[line_rows(k_self), :]

    inputs[2].wait()
    gate = jnp.zeros((n_exp, n_tok), F32)
    for j in range(n_top):
        gate = gate + jnp.where(idx_ref[j:j + 1, :] == row_e, gate_ref[j:j + 1, :], 0.0)
    gates[...] = gate

    with jax.named_scope('entry_wait'):
        pl.semaphore_wait(barrier, 4 * n_line - 3)

    inputs[1].wait()
    for m in MATES:
        mt_copy(m).start()
    for h in range(ahead):
        for m in (1, 3):
            gather_copy(m, h).start()

    xg[rows_at(k_self * n_tok, n_tok, 8), :] = x_ref[...]

    r = lax.broadcasted_iota(jnp.int32, (n_rows, 1), 0)
    r12 = div12(r)
    r_slot = (r - r12 * cap).astype(F32)
    r_src = r12 & (n_line - 1)
    r_dev = r12 >> 2
    e_lane = lax.broadcasted_iota(jnp.int32, (n_rows, n_line_exp), 1)
    with jax.named_scope('slots_wait'):
        wait_bytes(mts.at[pl.ds(0, n_line - 1)], mt_r.at[0])
    for l in range(n_loc):
        pick = (e_lane == n_loc * r_dev + l).astype(BF16)
        for s in range(n_line):
            val = dot(pick, mts[s])
            hit = jnp.logical_and(val == r_slot, r_src == s)
            sel[l, :, s * n_tok:(s + 1) * n_tok] = jnp.where(hit, 1.0, 0.0).astype(BF16)

    def spread(l, h):
        sendb[l, :, half_cols(h)] = dot(sel[l], xg[:, half_cols(h)]).astype(BF16)
        for m, dc in PEERS:
            spread_copy(l, h, m, dc).start()
        rows[l, rows_at(i_self * per, per, 8), half_cols(h)] = sendb[l, rows_at(d_self * per, per, 8), half_cols(h)]

    def relay(h):
        for m in (1, 3):
            gather_copy(m, h).wait_recv()
            relay_copy(m, h).start()

    def gathered(h):
        with jax.named_scope('gather_wait'):
            for m in (1, 3):
                relay_copy(m, h).wait_recv()
        with jax.named_scope('spread_send'):
            spread(0, h)

    with jax.named_scope('gather_and_spread'):
        for h in range(n_half):
            relay(h)
            if h + ahead < n_half:
                for m in (1, 3):
                    gather_copy(m, h + ahead).start()
            if h >= lead - 1:
                gathered(h - lead + 1)
        for m in (1, 3):
            for copy in note_copies(m):
                copy.start()
        for h in range(n_half - lead + 1, n_half):
            gathered(h)

    with jax.named_scope('spread_rest'):
        for h in range(n_half):
            for l in range(1, n_loc):
                spread(l, h)

    o12 = r12
    o_in = (o12 & 7) * per + (o12 >> 3) * cap + (r - r12 * cap)
    perm[...] = (lax.broadcasted_iota(jnp.int32, (n_rows, n_rows), 1) == o_in).astype(BF16)

    acc[...] = x_ref[...].astype(F32)

    def expert_up(l, cuts):
        with jax.named_scope('weight_wait'):
            for which in range(2):
                w13_copy(which, l).wait()
        edges = (0,) + cuts + (n_half,)
        for h0, h1 in zip(edges, edges[1:]):
            with jax.named_scope('spread_wait'):
                for h in range(h0, h1):
                    spread_wait(l, h)
            k = slice(h0 * half, h1 * half)

            def tile(n, carry, h0=h0, h1=h1, k=k):
                cols = pl.ds(pl.multiple_of(n * f_tile, f_tile), f_tile)
                a = dot(rows[l, :, k], w1[l, k, cols])
                b = dot(rows[l, :, k], w3[l, k, cols])
                if h0 > 0:
                    a = a + part_a[:, cols]
                    b = b + part_b[:, cols]
                if h1 < n_half:
                    part_a[:, cols] = a
                    part_b[:, cols] = b
                else:
                    hid[:, cols] = (jax.nn.silu(a) * b).astype(BF16)
                return carry

            with jax.named_scope('up'):
                lax.fori_loop(0, ffn // f_tile, tile, 0)

    def expert_down(l, c):
        t = l * n_chunk + c
        w2_copy(t).wait()
        rows[l, :, cols_at(c)] = dot(hid[...], w2[lax.rem(t, n_w2)]).astype(BF16)

        @pl.when(t + n_w2 < n_loc * n_chunk)
        def _():
            w2_copy(t + n_w2).start()

        for copy in back_copies(l, c):
            copy.start()
        y1[l, rows_at(d_self * per, per, 8), cols_at(c)] = rows[l, rows_at(i_self * per, per, 8), cols_at(c)]

    def forward(l, c):
        with jax.named_scope('back_wait'):
            back_wait(l, c)
        out = dot(perm[...], y1[l, :, cols_at(c)]).astype(BF16)
        for s in range(n_line):
            sendb[s >> 1, (s & 1) * both + l * home:(s & 1) * both + (l + 1) * home, cols_at(c)] = (
                out[s * home:(s + 1) * home])
        for m in (1, 3):
            far_copy(l, c, m).start()
        for m in (1, 3):
            raw_copy(l, c, m).start()

    def fold(v):
        return v[:n_tok] + v[n_tok:2 * n_tok] + v[2 * n_tok:]

    def home_rows(s):
        return s >> 1, rows_at((s & 1) * both, both, 8)

    def own_sums(c):
        p, r = home_rows(k_self)
        acc[:, cols_at(c)] += fold(dot(gmat[0], sendb[p, r, cols_at(c)]))
        for side, m in ((0, 3), (1, 1)):
            p, r = home_rows(mod(k_self + m))
            part_out[:, side_cols(c, side)] = fold(
                dot(sel[side, :, 0:both], sendb[p, r, side_cols(c, side)]))

    def merge(c):
        with jax.named_scope('far_wait'):
            wait_bytes(y_far.at[:, cols_at(c)], f_r.at[c])
        for side in range(2):
            cols = side_cols(c, side)
            part_out[:, cols] += fold(dot(sel[side, :, 256:256 + both], y_far[:, cols]))
        for m in (1, 3):
            sum_copy(c, m).start()

    def collect(c):
        with jax.named_scope('raw_wait'):
            wait_bytes(y_raw.at[:, cols_at(c)], e_r.at[c])
        for side in range(2):
            cols = side_cols(c, side)
            acc[:, cols] += fold(dot(gmat[1 + side], y_raw[:, cols]))

    def loop(body, start=0, stop=n_chunk):
        def step(c, carry):
            body(c)
            return carry
        lax.fori_loop(start, stop, step, 0)

    expert_up(0, cuts[0])
    with jax.named_scope('down0'):
        loop(lambda c: expert_down(0, c))
    expert_up(1, cuts[1])
    with jax.named_scope('spread_drain'):
        wait_bytes(sendb.at[:, pl.ds(0, others), :], d_s.at[0])

    def down_and_forward(c):
        expert_down(1, c)
        forward(0, c)

    with jax.named_scope('down1_forward0'):
        loop(down_and_forward)

    with jax.named_scope('gate_blocks'):
        eye = (lax.broadcasted_iota(jnp.int32, (n_tok, n_tok), 0)
               == lax.broadcasted_iota(jnp.int32, (n_tok, n_tok), 1)).astype(BF16)
        q = lax.broadcasted_iota(jnp.int32, (1, both), 1)
        q12 = div12(q)
        q_slot = (q - q12 * cap).astype(F32)
        q_exp = n_loc * (q12 & 7) + (q12 >> 3)
        spread_e = (lax.broadcasted_iota(jnp.int32, (n_line_exp, both), 0) == q_exp).astype(BF16)

        def gate_block(slot_rows, gate_rows, put):
            hit = dot(nt_dot(eye, slot_rows).astype(BF16), spread_e) == q_slot
            rest = gate_rows
            for p in range(3):
                part = rest.astype(BF16)
                rest = rest - part.astype(F32)
                put(p, jnp.where(hit, dot(nt_dot(eye, part).astype(BF16), spread_e), 0.0).astype(BF16))

        for n, m in enumerate((0, 3, 1)):
            k = line_rows(mod(k_self + m))

            def put_own(p, v, n=n):
                gmat[n, p * n_tok:(p + 1) * n_tok, :] = v

            gate_block(slots[k, :], gates[k, :], put_own)
        wait_bytes(slots_far, n_r.at[0])
        wait_bytes(gates_near, n_r.at[1])
        for side in range(2):
            for n in range(2):
                near = mts[mod(k_self + (3 if side == 0 else 1))] if n == 0 else slots_far[side]

                def put_near(p, v, side=side, n=n):
                    sel[side, p * n_tok:(p + 1) * n_tok, n * 256:n * 256 + both] = v

                gate_block(near, gates_near[side, n], put_near)
    def forward_and_sum(c):
        forward(1, c)
        own_sums(c)

    def forward_and_merge(c):
        forward_and_sum(c)
        merge(c - lag)

    with jax.named_scope('forward1'):
        loop(forward_and_sum, 0, lag)
        loop(forward_and_merge, lag, n_chunk)

    def merge_and_collect(c):
        merge(c)
        collect(c - n_chunk + lag)

    with jax.named_scope('merge'):
        loop(merge_and_collect, n_chunk - lag, n_chunk)
        loop(collect, lag, n_chunk)
    wait_bytes(xg.at[pl.ds(0, (n_line - 1) * n_tok), :], g_s.at[0])

    def finish(c):
        with jax.named_scope('sum_wait'):
            wait_bytes(part_in.at[:, cols_at(c)], p_r.at[c])
        out_ref[:, cols_at(c)] = (acc[:, cols_at(c)] + part_in[:, cols_at(c)]).astype(BF16)

    with jax.named_scope('finish'):
        loop(finish)

    with jax.named_scope('drain'):
        wait_bytes(mts.at[pl.ds(0, n_line - 1)], mt_s.at[0])
        wait_bytes(slots_far, n_s.at[0])
        wait_bytes(gates_near, n_s.at[1])
        wait_bytes(y1.at[:, pl.ds(0, others), :], c_s.at[0])
        wait_bytes(y1.at[0], e_s.at[0])
        wait_bytes(part_out, p_s.at[0])


def solution(mesh):
    group_axes = ('ep2', 'ep')
    n_line = mesh.shape['ep2']
    n_group = n_line * mesh.shape['ep']
    row_spec = P(('dp', 'ep2', 'ep'), None)
    weight_spec = P(group_axes, None, None)

    def device_step(tokens, expert_ids, gates, w_gate, w_up, w_down):
        n_tok, n_top = expert_ids.shape
        n_loc, dim, ffn = w_gate.shape
        n_exp = n_loc * n_group
        cap = -(-(n_tok * n_top) // n_exp)
        n_rows = n_group * cap
        n_half, n_chunk, f_tile, n_w2, cuts, ahead, lead, lag = 5, 5, 256, 3, ((2, 4), (2, 4)), 4, 3, 3
        sem = pltpu.SemaphoreType.DMA
        hbm = pl.BlockSpec(memory_space=pl.ANY)
        n_dev = 2 * n_line
        return pl.pallas_call(
            functools.partial(moe_kernel, n_line, cap, n_half, n_chunk, f_tile, cuts, ahead, lead, lag),
            out_shape=pltpu.VMEM((n_tok, dim), BF16),
            in_specs=[hbm] * 6,
            out_specs=pl.BlockSpec(memory_space=pltpu.VMEM),
            scratch_shapes=[
                pltpu.VMEM((n_tok, dim), BF16),
                pltpu.VMEM((n_top, n_tok), jnp.int32),
                pltpu.VMEM((n_top, n_tok), F32),
                pltpu.VMEM((n_loc, dim, ffn), BF16),
                pltpu.VMEM((n_loc, dim, ffn), BF16),
                pltpu.VMEM((n_w2, ffn, dim // n_chunk), BF16),
                pltpu.VMEM((n_exp, n_tok), BF16),
                pltpu.VMEM((n_exp, n_tok), F32),
                pltpu.VMEM((n_line, n_exp // n_line, n_tok), BF16),
                pltpu.VMEM((2, n_exp // n_line, n_tok), BF16),
                pltpu.VMEM((2, 2, n_exp // n_line, n_tok), F32),
                pltpu.VMEM((n_line * n_tok, dim), BF16),
                pltpu.VMEM((n_loc, n_rows, n_line * n_tok), BF16),
                pltpu.VMEM((n_loc, n_rows, dim), BF16),
                pltpu.VMEM((n_loc, n_rows, dim), BF16),
                pltpu.VMEM((n_rows, ffn), F32),
                pltpu.VMEM((n_rows, ffn), F32),
                pltpu.VMEM((n_rows, ffn), BF16),
                pltpu.VMEM((n_loc, n_rows, dim), BF16),
                pltpu.VMEM((n_loc * n_dev * cap, dim), BF16),
                pltpu.VMEM((n_loc * n_dev * cap, dim), BF16),
                pltpu.VMEM((n_rows, n_rows), BF16),
                pltpu.VMEM((3, 3 * n_tok, n_loc * n_dev * cap), BF16),
                pltpu.VMEM((n_tok, dim), F32),
                pltpu.VMEM((n_tok, dim), F32),
                pltpu.VMEM((n_tok, dim), F32),
                sem((3,)),
                sem((2, n_loc)),
                sem((n_w2,)),
                sem((1,)), sem((1,)),
                sem((2,)), sem((2,)),
                sem((1,)), sem((4, n_half)),
                sem((1,)), sem((n_loc, n_half)),
                sem((1,)), sem((n_loc, n_chunk)),
                sem((1,)), sem((n_chunk,)), sem((n_chunk,)),
                sem((1,)), sem((n_chunk,)),
            ],
            compiler_params=pltpu.CompilerParams(
                collective_id=0, has_side_effects=True, vmem_limit_bytes=66300000),
        )(tokens, expert_ids.T, gates.T, w_gate, w_up, w_down)

    return jax.shard_map(
        device_step, mesh=mesh,
        in_specs=(row_spec, row_spec, row_spec, weight_spec, weight_spec, weight_spec),
        out_specs=row_spec, check_vma=False)
```

```python
import functools

import jax
import jax.numpy as jnp
from jax import lax
from jax.experimental import pallas as pl
from jax.experimental.pallas import tpu as pltpu
from jax.sharding import PartitionSpec as P

MESH = pl.DeviceIdType.MESH
F32 = jnp.float32
BF16 = jnp.bfloat16
PEERS = [(2, 0), (2, 1), (1, 0), (3, 0), (1, 1), (3, 1), (0, 1)]
MATES = [1, 3, 2]


def div12(v):
    return (v * 2731) >> 15


def nt_dot(a, b):
    return lax.dot_general(a, b, (((1,), (1,)), ((), ())), preferred_element_type=F32)


def dot(a, b):
    return jnp.dot(a, b, preferred_element_type=F32)


def moe_kernel(
    n_line, cap, n_half, n_chunk, f_tile, cuts, ahead, lead, lag,
    x_hbm, idx_hbm, gate_hbm, w1_hbm, w3_hbm, w2_hbm, out_ref,
    x_ref, idx_ref, gate_ref, w1, w3, w2, slots, gates, mts, slots_far, gates_near, xg, sel, sendb, rows, part_a, part_b, hid, y1,
    y_raw, y_far, perm, gmat, acc, part_out, part_in,
    in_sem, w13_sem, w2_sem, mt_s, mt_r, n_s, n_r, g_s, g_r, d_s, d_r, c_s, c_r, e_s, e_r, f_r, p_s, p_r,
):
    n_tok, dim = x_ref.shape
    n_top = idx_ref.shape[0]
    n_loc, ffn = w2_hbm.shape[0], w2_hbm.shape[1]
    n_exp = slots.shape[0]
    n_line_exp = n_exp // n_line
    per = n_line * cap
    n_rows = 2 * n_line * per
    n_w2 = w2.shape[0]
    half = dim // n_half
    wide = dim // n_chunk

    dp = lax.axis_index('dp')
    yy = lax.axis_index('ep2')
    ee = lax.axis_index('ep')
    xx = ee // 2
    cc = lax.rem(ee, 2)
    k_self = jnp.where(cc == 0, yy, xx)
    q_self = jnp.where(cc == 0, xx, yy)
    i_self = cc * n_line + q_self
    d_self = 2 * q_self + cc
    coef_k = jnp.where(cc == 0, 16, 4)
    coef_q = jnp.where(cc == 0, 4, 16)

    def mod(v):
        return lax.rem(v + n_line, n_line)

    def mate(m):
        k = mod(k_self + m)
        return (dp, jnp.where(cc == 0, k, yy), jnp.where(cc == 0, xx, k) * 2 + cc)

    def spread_peer(m, dc):
        q = mod(q_self + m)
        c2 = lax.rem(cc + dc, 2)
        dev = (dp, jnp.where(cc == 0, yy, q), jnp.where(cc == 0, q, xx) * 2 + c2)
        return dev, 2 * q + c2

    def rows_at(start, size, unit):
        return pl.ds(pl.multiple_of(start, unit), size)

    def half_cols(h):
        return pl.ds(h * half, half)

    def cols_at(c):
        return pl.ds(pl.multiple_of(c * wide, wide), wide)

    def w13_copy(which, l):
        hbm, buf = ((w1_hbm, w1), (w3_hbm, w3))[which]
        return pltpu.make_async_copy(hbm.at[l], buf.at[l], w13_sem.at[which, l])

    def w2_copy(t):
        slot = lax.rem(t, n_w2)
        return pltpu.make_async_copy(
            w2_hbm.at[t // n_chunk, :, cols_at(lax.rem(t, n_chunk))], w2.at[slot], w2_sem.at[slot])

    def mt_copy(m):
        return pltpu.make_async_remote_copy(
            slots.at[line_rows(mod(k_self + m)), :], mts.at[k_self], mt_s.at[0], mt_r.at[0], device_id=mate(m), device_id_type=MESH)

    def gather_copy(m, h):
        return pltpu.make_async_remote_copy(
            x_ref.at[:, half_cols(h)], xg.at[rows_at(k_self * n_tok, n_tok, 8), half_cols(h)],
            g_s.at[0], g_r.at[m // 2, h], device_id=mate(m), device_id_type=MESH)

    def relay_copy(m, h):
        side = m // 2
        block = xg.at[rows_at(mod(k_self - m) * n_tok + side * (n_tok // 2), n_tok // 2, 8), half_cols(h)]
        return pltpu.make_async_remote_copy(
            block, block, g_s.at[0], g_r.at[2 + side, h], device_id=mate(m), device_id_type=MESH)

    def wait_bytes(ref, sem):
        pltpu.make_async_copy(ref, ref, sem).wait()

    def spread_copy(l, h, m, dc):
        dev, d = spread_peer(m, dc)
        return pltpu.make_async_remote_copy(
            sendb.at[l, rows_at(d * per, per, 8), half_cols(h)],
            rows.at[l, rows_at(i_self * per, per, 8), half_cols(h)],
            d_s.at[0], d_r.at[l, h], device_id=dev, device_id_type=MESH)

    others = (2 * n_line - 1) * per

    def spread_wait(l, h):
        wait_bytes(rows.at[l, pl.ds(0, others), half_cols(h)], d_r.at[l, h])

    def back_targets():
        out = []
        for m in (2, 1, 3):
            for side in (0, 1):
                pos = mod((yy if side else xx) + m)
                dev = (dp, pos, xx * 2 + 1) if side else (dp, yy, pos * 2)
                d_me = 2 * (yy if side else xx) + cc
                out.append((side * n_line + pos, dev, d_me))
        other = 1 - cc
        pos = jnp.where(other == 0, xx, yy)
        out.append((other * n_line + pos, (dp, yy, xx * 2 + other), 2 * pos + cc))
        return out

    def back_copies(l, c):
        return [
            pltpu.make_async_remote_copy(
                rows.at[l, rows_at(i * per, per, 8), cols_at(c)], y1.at[l, rows_at(d_me * per, per, 8), cols_at(c)],
                c_s.at[0], c_r.at[l, c], device_id=dev, device_id_type=MESH)
            for i, dev, d_me in back_targets()
        ]

    def back_wait(l, c):
        wait_bytes(y1.at[l, pl.ds(0, others), cols_at(c)], c_r.at[l, c])

    home = 2 * n_line * cap
    both = n_loc * home

    def at_home(s, l):
        return s >> 1, rows_at((s & 1) * both + l * home, home, 8)

    def side_cols(c, side):
        return pl.ds(pl.multiple_of(c * wide + side * (wide // 2), wide // 2), wide // 2)

    def raw_copy(l, c, m):
        side = m // 2
        p, r = at_home(mod(k_self + m), l)
        return pltpu.make_async_remote_copy(
            sendb.at[p, r, side_cols(c, side)], y_raw.at[pl.ds(l * home, home), side_cols(c, side)],
            e_s.at[0], e_r.at[c], device_id=mate(m), device_id_type=MESH)

    def far_copy(l, c, m):
        side = 1 - m // 2
        p, r = at_home(mod(k_self + 2), l)
        return pltpu.make_async_remote_copy(
            sendb.at[p, r, side_cols(c, side)], y_far.at[pl.ds(l * home, home), side_cols(c, side)],
            e_s.at[0], f_r.at[c], device_id=mate(m), device_id_type=MESH)

    def sum_copy(c, m):
        cols = side_cols(c, 1 - m // 2)
        return pltpu.make_async_remote_copy(
            part_out.at[:, cols], part_in.at[:, cols], p_s.at[0], p_r.at[c], device_id=mate(m), device_id_type=MESH)

    def line_rows(k):
        return pl.ds(pl.multiple_of(k * n_line_exp, n_line_exp), n_line_exp)

    def note_copies(m):
        side = m // 2
        out = [pltpu.make_async_remote_copy(
            slots.at[line_rows(mod(k_self + 2)), :], slots_far.at[side], n_s.at[0], n_r.at[0],
            device_id=mate(m), device_id_type=MESH)]
        for n, k in enumerate((mod(k_self + m), mod(k_self + 2))):
            out.append(pltpu.make_async_remote_copy(
                gates.at[line_rows(k), :], gates_near.at[side, n], n_s.at[1], n_r.at[1],
                device_id=mate(m), device_id_type=MESH))
        return out

    inputs = [
        pltpu.make_async_copy(src, dst, in_sem.at[n])
        for n, (src, dst) in enumerate(((idx_hbm, idx_ref), (x_hbm, x_ref), (gate_hbm, gate_ref)))
    ]
    for copy in inputs:
        copy.start()

    barrier = pltpu.get_barrier_semaphore()
    for side in (0, 1):
        for m in range(n_line):
            for dc in (0, 1):
                if (m, dc) == (0, 0) or (side and m == 0):
                    continue
                pos = mod((yy if side else xx) + m)
                c2 = lax.rem(cc + dc, 2)
                dev = (dp, pos, xx * 2 + c2) if side else (dp, yy, pos * 2 + c2)
                pl.semaphore_signal(barrier, inc=1, device_id=dev, device_id_type=MESH)

    for l in range(n_loc):
        for which in range(2):
            w13_copy(which, l).start()
    for t in range(n_w2):
        w2_copy(t).start()

    r_e = lax.broadcasted_iota(jnp.int32, (n_exp, n_tok), 0)
    row_e = (coef_k * (r_e >> 4) + coef_q * ((r_e >> 2) & 3) + (r_e & 3))
    inputs[0].wait()
    chosen = jnp.zeros((n_exp, n_tok), F32)
    for j in range(n_top):
        chosen = chosen + (idx_ref[j:j + 1, :] == row_e).astype(F32)
    before = (lax.broadcasted_iota(jnp.int32, (n_tok, n_tok), 0)
              < lax.broadcasted_iota(jnp.int32, (n_tok, n_tok), 1)).astype(BF16)
    slot = dot(chosen.astype(BF16), before)
    slot = jnp.where(chosen > 0, slot, -1.0).astype(BF16)
    slots[...] = slot
    mts[k_self] = slots[line_rows(k_self), :]

    inputs[2].wait()
    gate = jnp.zeros((n_exp, n_tok), F32)
    for j in range(n_top):
        gate = gate + jnp.where(idx_ref[j:j + 1, :] == row_e, gate_ref[j:j + 1, :], 0.0)
    gates[...] = gate

    with jax.named_scope('entry_wait'):
        pl.semaphore_wait(barrier, 4 * n_line - 3)

    inputs[1].wait()
    for m in MATES:
        mt_copy(m).start()
    for h in range(ahead):
        for m in (1, 3):
            gather_copy(m, h).start()

    xg[rows_at(k_self * n_tok, n_tok, 8), :] = x_ref[...]

    def relay(h):
        for m in (1, 3):
            gather_copy(m, h).wait_recv()
            relay_copy(m, h).start()

    relay(0)

    r = lax.broadcasted_iota(jnp.int32, (n_rows, 1), 0)
    r12 = div12(r)
    r_slot = (r - r12 * cap).astype(F32)
    r_src = r12 & (n_line - 1)
    r_dev = r12 >> 2
    e_lane = lax.broadcasted_iota(jnp.int32, (n_rows, n_line_exp), 1)
    with jax.named_scope('slots_wait'):
        wait_bytes(mts.at[pl.ds(0, n_line - 1)], mt_r.at[0])
    for l in range(n_loc):
        pick = (e_lane == n_loc * r_dev + l).astype(BF16)
        for s in range(n_line):
            val = dot(pick, mts[s])
            hit = jnp.logical_and(val == r_slot, r_src == s)
            sel[l, :, s * n_tok:(s + 1) * n_tok] = jnp.where(hit, 1.0, 0.0).astype(BF16)

    def spread(l, h):
        sendb[l, :, half_cols(h)] = dot(sel[l], xg[:, half_cols(h)]).astype(BF16)
        for m, dc in PEERS:
            spread_copy(l, h, m, dc).start()
        rows[l, rows_at(i_self * per, per, 8), half_cols(h)] = sendb[l, rows_at(d_self * per, per, 8), half_cols(h)]


    def gathered(h):
        with jax.named_scope('gather_wait'):
            for m in (1, 3):
                relay_copy(m, h).wait_recv()
        with jax.named_scope('spread_send'):
            spread(0, h)

    with jax.named_scope('gather_and_spread'):
        for h in range(n_half):
            if h > 0:
                relay(h)
            if h + ahead < n_half:
                for m in (1, 3):
                    gather_copy(m, h + ahead).start()
            if h >= lead - 1:
                gathered(h - lead + 1)
        for m in (1, 3):
            for copy in note_copies(m):
                copy.start()
        for h in range(n_half - lead + 1, n_half):
            gathered(h)

    with jax.named_scope('spread_rest'):
        for h in range(n_half):
            for l in range(1, n_loc):
                spread(l, h)

    o12 = r12
    o_in = (o12 & 7) * per + (o12 >> 3) * cap + (r - r12 * cap)
    perm[...] = (lax.broadcasted_iota(jnp.int32, (n_rows, n_rows), 1) == o_in).astype(BF16)

    acc[...] = x_ref[...].astype(F32)

    def expert_up(l, cuts):
        with jax.named_scope('weight_wait'):
            for which in range(2):
                w13_copy(which, l).wait()
        edges = (0,) + cuts + (n_half,)
        for h0, h1 in zip(edges, edges[1:]):
            with jax.named_scope('spread_wait'):
                for h in range(h0, h1):
                    spread_wait(l, h)
            k = slice(h0 * half, h1 * half)

            def tile(n, carry, h0=h0, h1=h1, k=k):
                cols = pl.ds(pl.multiple_of(n * f_tile, f_tile), f_tile)
                a = dot(rows[l, :, k], w1[l, k, cols])
                b = dot(rows[l, :, k], w3[l, k, cols])
                if h0 > 0:
                    a = a + part_a[:, cols]
                    b = b + part_b[:, cols]
                if h1 < n_half:
                    part_a[:, cols] = a
                    part_b[:, cols] = b
                else:
                    hid[:, cols] = (jax.nn.silu(a) * b).astype(BF16)
                return carry

            with jax.named_scope('up'):
                lax.fori_loop(0, ffn // f_tile, tile, 0)

    def expert_down(l, c):
        t = l * n_chunk + c
        w2_copy(t).wait()
        rows[l, :, cols_at(c)] = dot(hid[...], w2[lax.rem(t, n_w2)]).astype(BF16)

        @pl.when(t + n_w2 < n_loc * n_chunk)
        def _():
            w2_copy(t + n_w2).start()

        for copy in back_copies(l, c):
            copy.start()
        y1[l, rows_at(d_self * per, per, 8), cols_at(c)] = rows[l, rows_at(i_self * per, per, 8), cols_at(c)]

    def forward(l, c):
        with jax.named_scope('back_wait'):
            back_wait(l, c)
        out = dot(perm[...], y1[l, :, cols_at(c)]).astype(BF16)
        for s in range(n_line):
            sendb[s >> 1, (s & 1) * both + l * home:(s & 1) * both + (l + 1) * home, cols_at(c)] = (
                out[s * home:(s + 1) * home])
        for m in (1, 3):
            far_copy(l, c, m).start()
        for m in (1, 3):
            raw_copy(l, c, m).start()

    def fold(v):
        return v[:n_tok] + v[n_tok:2 * n_tok] + v[2 * n_tok:]

    def home_rows(s):
        return s >> 1, rows_at((s & 1) * both, both, 8)

    def own_sums(c):
        p, r = home_rows(k_self)
        acc[:, cols_at(c)] += fold(dot(gmat[0], sendb[p, r, cols_at(c)]))
        for side, m in ((0, 3), (1, 1)):
            p, r = home_rows(mod(k_self + m))
            part_out[:, side_cols(c, side)] = fold(
                dot(sel[side, :, 0:both], sendb[p, r, side_cols(c, side)]))

    def merge(c):
        with jax.named_scope('far_wait'):
            wait_bytes(y_far.at[:, cols_at(c)], f_r.at[c])
        for side in range(2):
            cols = side_cols(c, side)
            part_out[:, cols] += fold(dot(sel[side, :, 256:256 + both], y_far[:, cols]))
        for m in (1, 3):
            sum_copy(c, m).start()

    def collect(c):
        with jax.named_scope('raw_wait'):
            wait_bytes(y_raw.at[:, cols_at(c)], e_r.at[c])
        for side in range(2):
            cols = side_cols(c, side)
            acc[:, cols] += fold(dot(gmat[1 + side], y_raw[:, cols]))

    def loop(body, start=0, stop=n_chunk):
        def step(c, carry):
            body(c)
            return carry
        lax.fori_loop(start, stop, step, 0)

    expert_up(0, cuts[0])
    with jax.named_scope('down0'):
        loop(lambda c: expert_down(0, c))
    expert_up(1, cuts[1])
    with jax.named_scope('spread_drain'):
        wait_bytes(sendb.at[:, pl.ds(0, others), :], d_s.at[0])

    def down_and_forward(c):
        expert_down(1, c)
        forward(0, c)

    with jax.named_scope('down1_forward0'):
        loop(down_and_forward)

    with jax.named_scope('gate_blocks'):
        eye = (lax.broadcasted_iota(jnp.int32, (n_tok, n_tok), 0)
               == lax.broadcasted_iota(jnp.int32, (n_tok, n_tok), 1)).astype(BF16)
        q = lax.broadcasted_iota(jnp.int32, (1, both), 1)
        q12 = div12(q)
        q_slot = (q - q12 * cap).astype(F32)
        q_exp = n_loc * (q12 & 7) + (q12 >> 3)
        spread_e = (lax.broadcasted_iota(jnp.int32, (n_line_exp, both), 0) == q_exp).astype(BF16)

        def gate_block(slot_rows, gate_rows, put):
            hit = dot(nt_dot(eye, slot_rows).astype(BF16), spread_e) == q_slot
            rest = gate_rows
            for p in range(3):
                part = rest.astype(BF16)
                rest = rest - part.astype(F32)
                put(p, jnp.where(hit, dot(nt_dot(eye, part).astype(BF16), spread_e), 0.0).astype(BF16))

        for n, m in enumerate((0, 3, 1)):
            k = line_rows(mod(k_self + m))

            def put_own(p, v, n=n):
                gmat[n, p * n_tok:(p + 1) * n_tok, :] = v

            gate_block(slots[k, :], gates[k, :], put_own)
        wait_bytes(slots_far, n_r.at[0])
        wait_bytes(gates_near, n_r.at[1])
        for side in range(2):
            for n in range(2):
                near = mts[mod(k_self + (3 if side == 0 else 1))] if n == 0 else slots_far[side]

                def put_near(p, v, side=side, n=n):
                    sel[side, p * n_tok:(p + 1) * n_tok, n * 256:n * 256 + both] = v

                gate_block(near, gates_near[side, n], put_near)
    def forward_and_sum(c):
        forward(1, c)
        own_sums(c)

    def forward_and_merge(c):
        forward_and_sum(c)
        merge(c - lag)

    with jax.named_scope('forward1'):
        loop(forward_and_sum, 0, lag)
        loop(forward_and_merge, lag, n_chunk)

    def merge_and_collect(c):
        merge(c)
        collect(c - n_chunk + lag)

    with jax.named_scope('merge'):
        loop(merge_and_collect, n_chunk - lag, n_chunk)
        loop(collect, lag, n_chunk)
    wait_bytes(xg.at[pl.ds(0, (n_line - 1) * n_tok), :], g_s.at[0])

    def finish(c):
        with jax.named_scope('sum_wait'):
            wait_bytes(part_in.at[:, cols_at(c)], p_r.at[c])
        out_ref[:, cols_at(c)] = (acc[:, cols_at(c)] + part_in[:, cols_at(c)]).astype(BF16)

    with jax.named_scope('finish'):
        loop(finish)

    with jax.named_scope('drain'):
        wait_bytes(mts.at[pl.ds(0, n_line - 1)], mt_s.at[0])
        wait_bytes(slots_far, n_s.at[0])
        wait_bytes(gates_near, n_s.at[1])
        wait_bytes(y1.at[:, pl.ds(0, others), :], c_s.at[0])
        wait_bytes(y1.at[0], e_s.at[0])
        wait_bytes(part_out, p_s.at[0])


def solution(mesh):
    group_axes = ('ep2', 'ep')
    n_line = mesh.shape['ep2']
    n_group = n_line * mesh.shape['ep']
    row_spec = P(('dp', 'ep2', 'ep'), None)
    weight_spec = P(group_axes, None, None)

    def device_step(tokens, expert_ids, gates, w_gate, w_up, w_down):
        n_tok, n_top = expert_ids.shape
        n_loc, dim, ffn = w_gate.shape
        n_exp = n_loc * n_group
        cap = -(-(n_tok * n_top) // n_exp)
        n_rows = n_group * cap
        n_half, n_chunk, f_tile, n_w2, cuts, ahead, lead, lag = 5, 5, 256, 3, ((2, 4), (2, 4)), 4, 3, 3
        sem = pltpu.SemaphoreType.DMA
        hbm = pl.BlockSpec(memory_space=pl.ANY)
        n_dev = 2 * n_line
        return pl.pallas_call(
            functools.partial(moe_kernel, n_line, cap, n_half, n_chunk, f_tile, cuts, ahead, lead, lag),
            out_shape=pltpu.VMEM((n_tok, dim), BF16),
            in_specs=[hbm] * 6,
            out_specs=pl.BlockSpec(memory_space=pltpu.VMEM),
            scratch_shapes=[
                pltpu.VMEM((n_tok, dim), BF16),
                pltpu.VMEM((n_top, n_tok), jnp.int32),
                pltpu.VMEM((n_top, n_tok), F32),
                pltpu.VMEM((n_loc, dim, ffn), BF16),
                pltpu.VMEM((n_loc, dim, ffn), BF16),
                pltpu.VMEM((n_w2, ffn, dim // n_chunk), BF16),
                pltpu.VMEM((n_exp, n_tok), BF16),
                pltpu.VMEM((n_exp, n_tok), F32),
                pltpu.VMEM((n_line, n_exp // n_line, n_tok), BF16),
                pltpu.VMEM((2, n_exp // n_line, n_tok), BF16),
                pltpu.VMEM((2, 2, n_exp // n_line, n_tok), F32),
                pltpu.VMEM((n_line * n_tok, dim), BF16),
                pltpu.VMEM((n_loc, n_rows, n_line * n_tok), BF16),
                pltpu.VMEM((n_loc, n_rows, dim), BF16),
                pltpu.VMEM((n_loc, n_rows, dim), BF16),
                pltpu.VMEM((n_rows, ffn), F32),
                pltpu.VMEM((n_rows, ffn), F32),
                pltpu.VMEM((n_rows, ffn), BF16),
                pltpu.VMEM((n_loc, n_rows, dim), BF16),
                pltpu.VMEM((n_loc * n_dev * cap, dim), BF16),
                pltpu.VMEM((n_loc * n_dev * cap, dim), BF16),
                pltpu.VMEM((n_rows, n_rows), BF16),
                pltpu.VMEM((3, 3 * n_tok, n_loc * n_dev * cap), BF16),
                pltpu.VMEM((n_tok, dim), F32),
                pltpu.VMEM((n_tok, dim), F32),
                pltpu.VMEM((n_tok, dim), F32),
                sem((3,)),
                sem((2, n_loc)),
                sem((n_w2,)),
                sem((1,)), sem((1,)),
                sem((2,)), sem((2,)),
                sem((1,)), sem((4, n_half)),
                sem((1,)), sem((n_loc, n_half)),
                sem((1,)), sem((n_loc, n_chunk)),
                sem((1,)), sem((n_chunk,)), sem((n_chunk,)),
                sem((1,)), sem((n_chunk,)),
            ],
            compiler_params=pltpu.CompilerParams(
                collective_id=0, has_side_effects=True, vmem_limit_bytes=66300000),
        )(tokens, expert_ids.T, gates.T, w_gate, w_up, w_down)

    return jax.shard_map(
        device_step, mesh=mesh,
        in_specs=(row_spec, row_spec, row_spec, weight_spec, weight_spec, weight_spec),
        out_specs=row_spec, check_vma=False)
```

```python
import functools

import jax
import jax.numpy as jnp
from jax import lax
from jax.experimental import pallas as pl
from jax.experimental.pallas import tpu as pltpu
from jax.sharding import PartitionSpec as P

MESH = pl.DeviceIdType.MESH
F32 = jnp.float32
BF16 = jnp.bfloat16
BF16_MAX = float(jnp.finfo(jnp.bfloat16).max)
PEERS = [(2, 0), (2, 1), (1, 0), (3, 0), (1, 1), (3, 1), (0, 1)]
MATES = [1, 3, 2]


def div12(v):
    return (v * 2731) >> 15


def nt_dot(a, b):
    return lax.dot_general(a, b, (((1,), (1,)), ((), ())), preferred_element_type=F32)


def dot(a, b):
    return jnp.dot(a, b, preferred_element_type=F32)


def moe_kernel(
    n_line, cap, n_half, n_chunk, f_tile, cuts, ahead, lead, lag,
    x_hbm, idx_hbm, gate_hbm, w1_hbm, w3_hbm, w2_hbm, out_ref,
    x_ref, idx_ref, gate_ref, w1, w3, w2, slots, gates, mts, slots_far, gates_near, xg, sel, sendb, rows, part_a, part_b, hid, y1,
    y_raw, y_far, perm, gmat, acc, part_out, part_in,
    in_sem, w13_sem, w2_sem, mt_s, mt_r, n_s, n_r, g_s, g_r, d_s, d_r, c_s, c_r, e_s, e_r, f_r, p_s, p_r,
):
    n_tok, dim = x_ref.shape
    n_top = idx_ref.shape[0]
    n_loc, ffn = w2_hbm.shape[0], w2_hbm.shape[1]
    n_exp = slots.shape[0]
    n_line_exp = n_exp // n_line
    per = n_line * cap
    n_rows = 2 * n_line * per
    n_w2 = w2.shape[0]
    half = dim // n_half
    wide = dim // n_chunk

    dp = lax.axis_index('dp')
    yy = lax.axis_index('ep2')
    ee = lax.axis_index('ep')
    xx = ee // 2
    cc = lax.rem(ee, 2)
    k_self = jnp.where(cc == 0, yy, xx)
    q_self = jnp.where(cc == 0, xx, yy)
    i_self = cc * n_line + q_self
    d_self = 2 * q_self + cc
    coef_k = jnp.where(cc == 0, 16, 4)
    coef_q = jnp.where(cc == 0, 4, 16)

    def mod(v):
        return lax.rem(v + n_line, n_line)

    def mate(m):
        k = mod(k_self + m)
        return (dp, jnp.where(cc == 0, k, yy), jnp.where(cc == 0, xx, k) * 2 + cc)

    def spread_peer(m, dc):
        q = mod(q_self + m)
        c2 = lax.rem(cc + dc, 2)
        dev = (dp, jnp.where(cc == 0, yy, q), jnp.where(cc == 0, q, xx) * 2 + c2)
        return dev, 2 * q + c2

    def rows_at(start, size, unit):
        return pl.ds(pl.multiple_of(start, unit), size)

    def half_cols(h):
        return pl.ds(h * half, half)

    def cols_at(c):
        return pl.ds(pl.multiple_of(c * wide, wide), wide)

    def w13_copy(which, l):
        hbm, buf = ((w1_hbm, w1), (w3_hbm, w3))[which]
        return pltpu.make_async_copy(hbm.at[l], buf.at[l], w13_sem.at[which, l])

    def w2_copy(t):
        slot = lax.rem(t, n_w2)
        return pltpu.make_async_copy(
            w2_hbm.at[t // n_chunk, :, cols_at(lax.rem(t, n_chunk))], w2.at[slot], w2_sem.at[slot])

    def mt_copy(m):
        return pltpu.make_async_remote_copy(
            slots.at[line_rows(mod(k_self + m)), :], mts.at[k_self], mt_s.at[0], mt_r.at[0], device_id=mate(m), device_id_type=MESH)

    def gather_copy(m, h):
        return pltpu.make_async_remote_copy(
            x_ref.at[:, half_cols(h)], xg.at[rows_at(k_self * n_tok, n_tok, 8), half_cols(h)],
            g_s.at[0], g_r.at[m // 2, h], device_id=mate(m), device_id_type=MESH)

    def relay_copy(m, h):
        side = m // 2
        block = xg.at[rows_at(mod(k_self - m) * n_tok + side * (n_tok // 2), n_tok // 2, 8), half_cols(h)]
        return pltpu.make_async_remote_copy(
            block, block, g_s.at[0], g_r.at[2 + side, h], device_id=mate(m), device_id_type=MESH)

    def wait_bytes(ref, sem):
        pltpu.make_async_copy(ref, ref, sem).wait()

    def spread_copy(l, h, m, dc):
        dev, d = spread_peer(m, dc)
        return pltpu.make_async_remote_copy(
            sendb.at[l, rows_at(d * per, per, 8), half_cols(h)],
            rows.at[l, rows_at(i_self * per, per, 8), half_cols(h)],
            d_s.at[0], d_r.at[l, h], device_id=dev, device_id_type=MESH)

    others = (2 * n_line - 1) * per

    def spread_wait(l, h):
        wait_bytes(rows.at[l, pl.ds(0, others), half_cols(h)], d_r.at[l, h])

    def back_targets():
        out = []
        for m in (2, 1, 3):
            for side in (0, 1):
                pos = mod((yy if side else xx) + m)
                dev = (dp, pos, xx * 2 + 1) if side else (dp, yy, pos * 2)
                d_me = 2 * (yy if side else xx) + cc
                out.append((side * n_line + pos, dev, d_me))
        other = 1 - cc
        pos = jnp.where(other == 0, xx, yy)
        out.append((other * n_line + pos, (dp, yy, xx * 2 + other), 2 * pos + cc))
        return out

    def back_copies(l, c):
        return [
            pltpu.make_async_remote_copy(
                rows.at[l, rows_at(i * per, per, 8), cols_at(c)], y1.at[l, rows_at(d_me * per, per, 8), cols_at(c)],
                c_s.at[0], c_r.at[l, c], device_id=dev, device_id_type=MESH)
            for i, dev, d_me in back_targets()
        ]

    def back_wait(l, c):
        wait_bytes(y1.at[l, pl.ds(0, others), cols_at(c)], c_r.at[l, c])

    home = 2 * n_line * cap
    both = n_loc * home

    def at_home(s, l):
        return s >> 1, rows_at((s & 1) * both + l * home, home, 8)

    def side_cols(c, side):
        return pl.ds(pl.multiple_of(c * wide + side * (wide // 2), wide // 2), wide // 2)

    def raw_copy(l, c, m):
        side = m // 2
        p, r = at_home(mod(k_self + m), l)
        return pltpu.make_async_remote_copy(
            sendb.at[p, r, side_cols(c, side)], y_raw.at[pl.ds(l * home, home), side_cols(c, side)],
            e_s.at[0], e_r.at[c], device_id=mate(m), device_id_type=MESH)

    def far_copy(l, c, m):
        side = 1 - m // 2
        p, r = at_home(mod(k_self + 2), l)
        return pltpu.make_async_remote_copy(
            sendb.at[p, r, side_cols(c, side)], y_far.at[pl.ds(l * home, home), side_cols(c, side)],
            e_s.at[0], f_r.at[c], device_id=mate(m), device_id_type=MESH)

    def sum_copy(c, m):
        cols = side_cols(c, 1 - m // 2)
        return pltpu.make_async_remote_copy(
            part_out.at[:, cols], part_in.at[:, cols], p_s.at[0], p_r.at[c], device_id=mate(m), device_id_type=MESH)

    def line_rows(k):
        return pl.ds(pl.multiple_of(k * n_line_exp, n_line_exp), n_line_exp)

    def note_copies(m):
        side = m // 2
        out = [pltpu.make_async_remote_copy(
            slots.at[line_rows(mod(k_self + 2)), :], slots_far.at[side], n_s.at[0], n_r.at[0],
            device_id=mate(m), device_id_type=MESH)]
        for n, k in enumerate((mod(k_self + m), mod(k_self + 2))):
            out.append(pltpu.make_async_remote_copy(
                gates.at[line_rows(k), :], gates_near.at[side, n], n_s.at[1], n_r.at[1],
                device_id=mate(m), device_id_type=MESH))
        return out

    inputs = [
        pltpu.make_async_copy(src, dst, in_sem.at[n])
        for n, (src, dst) in enumerate(((idx_hbm, idx_ref), (x_hbm, x_ref), (gate_hbm, gate_ref)))
    ]
    for copy in inputs:
        copy.start()

    barrier = pltpu.get_barrier_semaphore()
    for side in (0, 1):
        for m in range(n_line):
            for dc in (0, 1):
                if (m, dc) == (0, 0) or (side and m == 0):
                    continue
                pos = mod((yy if side else xx) + m)
                c2 = lax.rem(cc + dc, 2)
                dev = (dp, pos, xx * 2 + c2) if side else (dp, yy, pos * 2 + c2)
                pl.semaphore_signal(barrier, inc=1, device_id=dev, device_id_type=MESH)

    for l in range(n_loc):
        for which in range(2):
            w13_copy(which, l).start()
    for t in range(n_w2):
        w2_copy(t).start()

    r_e = lax.broadcasted_iota(jnp.int32, (n_exp, n_tok), 0)
    row_e = (coef_k * (r_e >> 4) + coef_q * ((r_e >> 2) & 3) + (r_e & 3))
    inputs[0].wait()
    chosen = jnp.zeros((n_exp, n_tok), F32)
    for j in range(n_top):
        chosen = chosen + (idx_ref[j:j + 1, :] == row_e).astype(F32)
    before = (lax.broadcasted_iota(jnp.int32, (n_tok, n_tok), 0)
              < lax.broadcasted_iota(jnp.int32, (n_tok, n_tok), 1)).astype(BF16)
    slot = dot(chosen.astype(BF16), before)
    slot = jnp.where(chosen > 0, slot, -1.0).astype(BF16)
    slots[...] = slot
    mts[k_self] = slots[line_rows(k_self), :]

    inputs[2].wait()
    gate = jnp.zeros((n_exp, n_tok), F32)
    for j in range(n_top):
        gate = gate + jnp.where(idx_ref[j:j + 1, :] == row_e, gate_ref[j:j + 1, :], 0.0)
    gates[...] = gate

    with jax.named_scope('entry_wait'):
        pl.semaphore_wait(barrier, 4 * n_line - 3)

    inputs[1].wait()
    for m in MATES:
        mt_copy(m).start()
    for h in range(ahead):
        for m in (1, 3):
            gather_copy(m, h).start()

    xg[rows_at(k_self * n_tok, n_tok, 8), :] = x_ref[...]

    def relay(h):
        for m in (1, 3):
            gather_copy(m, h).wait_recv()
            relay_copy(m, h).start()

    relay(0)

    r = lax.broadcasted_iota(jnp.int32, (n_rows, 1), 0)
    r12 = div12(r)
    r_slot = (r - r12 * cap).astype(F32)
    r_src = r12 & (n_line - 1)
    r_dev = r12 >> 2
    e_lane = lax.broadcasted_iota(jnp.int32, (n_rows, n_line_exp), 1)
    with jax.named_scope('slots_wait'):
        wait_bytes(mts.at[pl.ds(0, n_line - 1)], mt_r.at[0])
    for l in range(n_loc):
        pick = (e_lane == n_loc * r_dev + l).astype(BF16)
        for s in range(n_line):
            val = dot(pick, mts[s])
            hit = jnp.logical_and(val == r_slot, r_src == s)
            sel[l, :, s * n_tok:(s + 1) * n_tok] = jnp.where(hit, 1.0, 0.0).astype(BF16)

    def spread(l, h):
        sendb[l, :, half_cols(h)] = dot(sel[l], xg[:, half_cols(h)]).astype(BF16)
        for m, dc in PEERS:
            spread_copy(l, h, m, dc).start()
        rows[l, rows_at(i_self * per, per, 8), half_cols(h)] = sendb[l, rows_at(d_self * per, per, 8), half_cols(h)]


    def gathered(h):
        with jax.named_scope('gather_wait'):
            for m in (1, 3):
                relay_copy(m, h).wait_recv()
        with jax.named_scope('spread_send'):
            spread(0, h)

    with jax.named_scope('gather_and_spread'):
        for h in range(n_half):
            if h > 0:
                relay(h)
            if h + ahead < n_half:
                for m in (1, 3):
                    gather_copy(m, h + ahead).start()
            if h >= lead - 1:
                gathered(h - lead + 1)
        for m in (1, 3):
            for copy in note_copies(m):
                copy.start()
        for h in range(n_half - lead + 1, n_half):
            gathered(h)

    with jax.named_scope('spread_rest'):
        for h in range(n_half):
            for l in range(1, n_loc):
                spread(l, h)

    o12 = r12
    o_in = (o12 & 7) * per + (o12 >> 3) * cap + (r - r12 * cap)
    perm[...] = (lax.broadcasted_iota(jnp.int32, (n_rows, n_rows), 1) == o_in).astype(BF16)

    acc[...] = x_ref[...].astype(F32)

    def expert_up(l, cuts):
        with jax.named_scope('weight_wait'):
            for which in range(2):
                w13_copy(which, l).wait()
        edges = (0,) + cuts + (n_half,)
        for h0, h1 in zip(edges, edges[1:]):
            with jax.named_scope('spread_wait'):
                for h in range(h0, h1):
                    spread_wait(l, h)
            k = slice(h0 * half, h1 * half)

            def tile(n, carry, h0=h0, h1=h1, k=k):
                cols = pl.ds(pl.multiple_of(n * f_tile, f_tile), f_tile)
                a = dot(rows[l, :, k], w1[l, k, cols])
                b = dot(rows[l, :, k], w3[l, k, cols])
                if h0 > 0:
                    a = a + part_a[:, cols]
                    b = b + part_b[:, cols]
                if h1 < n_half:
                    part_a[:, cols] = a
                    part_b[:, cols] = b
                else:
                    hid[:, cols] = (jax.nn.silu(a) * b).astype(BF16)
                return carry

            with jax.named_scope('up'):
                lax.fori_loop(0, ffn // f_tile, tile, 0)

    def expert_down(l, c):
        t = l * n_chunk + c
        w2_copy(t).wait()
        rows[l, :, cols_at(c)] = dot(hid[...], w2[lax.rem(t, n_w2)]).astype(BF16)

        @pl.when(t + n_w2 < n_loc * n_chunk)
        def _():
            w2_copy(t + n_w2).start()

        for copy in back_copies(l, c):
            copy.start()
        y1[l, rows_at(d_self * per, per, 8), cols_at(c)] = rows[l, rows_at(i_self * per, per, 8), cols_at(c)]

    def forward(l, c):
        with jax.named_scope('back_wait'):
            back_wait(l, c)
        out = dot(perm[...], y1[l, :, cols_at(c)]).astype(BF16)
        for s in range(n_line):
            sendb[s >> 1, (s & 1) * both + l * home:(s & 1) * both + (l + 1) * home, cols_at(c)] = (
                out[s * home:(s + 1) * home])
        for m in (1, 3):
            far_copy(l, c, m).start()
        for m in (1, 3):
            raw_copy(l, c, m).start()

    def fold(v):
        return v[:n_tok] + v[n_tok:2 * n_tok] + v[2 * n_tok:]

    def home_rows(s):
        return s >> 1, rows_at((s & 1) * both, both, 8)

    def own_sums(c):
        p, r = home_rows(k_self)
        acc[:, cols_at(c)] += fold(dot(gmat[0], sendb[p, r, cols_at(c)]))
        for side, m in ((0, 3), (1, 1)):
            p, r = home_rows(mod(k_self + m))
            part_out[:, side_cols(c, side)] = fold(
                dot(sel[side, :, 0:both], sendb[p, r, side_cols(c, side)]))

    def merge(c):
        with jax.named_scope('far_wait'):
            wait_bytes(y_far.at[:, cols_at(c)], f_r.at[c])
        for side in range(2):
            cols = side_cols(c, side)
            part_out[:, cols] += fold(dot(sel[side, :, 256:256 + both], y_far[:, cols]))
        for m in (1, 3):
            sum_copy(c, m).start()

    def collect(c):
        with jax.named_scope('raw_wait'):
            wait_bytes(y_raw.at[:, cols_at(c)], e_r.at[c])
        for side in range(2):
            cols = side_cols(c, side)
            acc[:, cols] += fold(dot(gmat[1 + side], y_raw[:, cols]))

    def loop(body, start=0, stop=n_chunk):
        def step(c, carry):
            body(c)
            return carry
        lax.fori_loop(start, stop, step, 0)

    expert_up(0, cuts[0])
    with jax.named_scope('down0'):
        loop(lambda c: expert_down(0, c))
    expert_up(1, cuts[1])
    with jax.named_scope('spread_drain'):
        wait_bytes(sendb.at[:, pl.ds(0, others), :], d_s.at[0])

    def down_and_forward(c):
        expert_down(1, c)
        forward(0, c)

    with jax.named_scope('down1_forward0'):
        loop(down_and_forward)

    with jax.named_scope('gate_blocks'):
        eye = (lax.broadcasted_iota(jnp.int32, (n_tok, n_tok), 0)
               == lax.broadcasted_iota(jnp.int32, (n_tok, n_tok), 1)).astype(BF16)
        q = lax.broadcasted_iota(jnp.int32, (1, both), 1)
        q12 = div12(q)
        q_slot = (q - q12 * cap).astype(F32)
        q_exp = n_loc * (q12 & 7) + (q12 >> 3)
        spread_e = (lax.broadcasted_iota(jnp.int32, (n_line_exp, both), 0) == q_exp).astype(BF16)

        def gate_block(slot_rows, gate_rows, put):
            hit = dot(nt_dot(eye, slot_rows).astype(BF16), spread_e) == q_slot
            rest = gate_rows
            for p in range(3):
                part = jnp.minimum(rest, BF16_MAX).astype(BF16)
                rest = rest - part.astype(F32)
                put(p, jnp.where(hit, dot(nt_dot(eye, part).astype(BF16), spread_e), 0.0).astype(BF16))

        for n, m in enumerate((0, 3, 1)):
            k = line_rows(mod(k_self + m))

            def put_own(p, v, n=n):
                gmat[n, p * n_tok:(p + 1) * n_tok, :] = v

            gate_block(slots[k, :], gates[k, :], put_own)
        wait_bytes(slots_far, n_r.at[0])
        wait_bytes(gates_near, n_r.at[1])
        for side in range(2):
            for n in range(2):
                near = mts[mod(k_self + (3 if side == 0 else 1))] if n == 0 else slots_far[side]

                def put_near(p, v, side=side, n=n):
                    sel[side, p * n_tok:(p + 1) * n_tok, n * 256:n * 256 + both] = v

                gate_block(near, gates_near[side, n], put_near)
    def forward_and_sum(c):
        forward(1, c)
        own_sums(c)

    def forward_and_merge(c):
        forward_and_sum(c)
        merge(c - lag)

    with jax.named_scope('forward1'):
        loop(forward_and_sum, 0, lag)
        loop(forward_and_merge, lag, n_chunk)

    def merge_and_collect(c):
        merge(c)
        collect(c - n_chunk + lag)

    with jax.named_scope('merge'):
        loop(merge_and_collect, n_chunk - lag, n_chunk)
        loop(collect, lag, n_chunk)
    wait_bytes(xg.at[pl.ds(0, (n_line - 1) * n_tok), :], g_s.at[0])

    def finish(c):
        with jax.named_scope('sum_wait'):
            wait_bytes(part_in.at[:, cols_at(c)], p_r.at[c])
        out_ref[:, cols_at(c)] = (acc[:, cols_at(c)] + part_in[:, cols_at(c)]).astype(BF16)

    with jax.named_scope('finish'):
        loop(finish)

    with jax.named_scope('drain'):
        wait_bytes(mts.at[pl.ds(0, n_line - 1)], mt_s.at[0])
        wait_bytes(slots_far, n_s.at[0])
        wait_bytes(gates_near, n_s.at[1])
        wait_bytes(y1.at[:, pl.ds(0, others), :], c_s.at[0])
        wait_bytes(y1.at[0], e_s.at[0])
        wait_bytes(part_out, p_s.at[0])


def solution(mesh):
    group_axes = ('ep2', 'ep')
    n_line = mesh.shape['ep2']
    n_group = n_line * mesh.shape['ep']
    row_spec = P(('dp', 'ep2', 'ep'), None)
    weight_spec = P(group_axes, None, None)

    def device_step(tokens, expert_ids, gates, w_gate, w_up, w_down):
        n_tok, n_top = expert_ids.shape
        n_loc, dim, ffn = w_gate.shape
        n_exp = n_loc * n_group
        cap = -(-(n_tok * n_top) // n_exp)
        n_rows = n_group * cap
        n_half, n_chunk, f_tile, n_w2, cuts, ahead, lead, lag = 5, 5, 256, 3, ((2, 4), (2, 4)), 4, 3, 3
        sem = pltpu.SemaphoreType.DMA
        hbm = pl.BlockSpec(memory_space=pl.ANY)
        n_dev = 2 * n_line
        return pl.pallas_call(
            functools.partial(moe_kernel, n_line, cap, n_half, n_chunk, f_tile, cuts, ahead, lead, lag),
            out_shape=pltpu.VMEM((n_tok, dim), BF16),
            in_specs=[hbm] * 6,
            out_specs=pl.BlockSpec(memory_space=pltpu.VMEM),
            scratch_shapes=[
                pltpu.VMEM((n_tok, dim), BF16),
                pltpu.VMEM((n_top, n_tok), jnp.int32),
                pltpu.VMEM((n_top, n_tok), F32),
                pltpu.VMEM((n_loc, dim, ffn), BF16),
                pltpu.VMEM((n_loc, dim, ffn), BF16),
                pltpu.VMEM((n_w2, ffn, dim // n_chunk), BF16),
                pltpu.VMEM((n_exp, n_tok), BF16),
                pltpu.VMEM((n_exp, n_tok), F32),
                pltpu.VMEM((n_line, n_exp // n_line, n_tok), BF16),
                pltpu.VMEM((2, n_exp // n_line, n_tok), BF16),
                pltpu.VMEM((2, 2, n_exp // n_line, n_tok), F32),
                pltpu.VMEM((n_line * n_tok, dim), BF16),
                pltpu.VMEM((n_loc, n_rows, n_line * n_tok), BF16),
                pltpu.VMEM((n_loc, n_rows, dim), BF16),
                pltpu.VMEM((n_loc, n_rows, dim), BF16),
                pltpu.VMEM((n_rows, ffn), F32),
                pltpu.VMEM((n_rows, ffn), F32),
                pltpu.VMEM((n_rows, ffn), BF16),
                pltpu.VMEM((n_loc, n_rows, dim), BF16),
                pltpu.VMEM((n_loc * n_dev * cap, dim), BF16),
                pltpu.VMEM((n_loc * n_dev * cap, dim), BF16),
                pltpu.VMEM((n_rows, n_rows), BF16),
                pltpu.VMEM((3, 3 * n_tok, n_loc * n_dev * cap), BF16),
                pltpu.VMEM((n_tok, dim), F32),
                pltpu.VMEM((n_tok, dim), F32),
                pltpu.VMEM((n_tok, dim), F32),
                sem((3,)),
                sem((2, n_loc)),
                sem((n_w2,)),
                sem((1,)), sem((1,)),
                sem((2,)), sem((2,)),
                sem((1,)), sem((4, n_half)),
                sem((1,)), sem((n_loc, n_half)),
                sem((1,)), sem((n_loc, n_chunk)),
                sem((1,)), sem((n_chunk,)), sem((n_chunk,)),
                sem((1,)), sem((n_chunk,)),
            ],
            compiler_params=pltpu.CompilerParams(
                collective_id=0, has_side_effects=True, vmem_limit_bytes=66300000),
        )(tokens, expert_ids.T, gates.T, w_gate, w_up, w_down)

    return jax.shard_map(
        device_step, mesh=mesh,
        in_specs=(row_spec, row_spec, row_spec, weight_spec, weight_spec, weight_spec),
        out_specs=row_spec, check_vma=False)
```

```python
import functools

import jax
import jax.numpy as jnp
from jax import lax
from jax.experimental import pallas as pl
from jax.experimental.pallas import tpu as pltpu
from jax.sharding import PartitionSpec as P

MESH = pl.DeviceIdType.MESH
F32 = jnp.float32
BF16 = jnp.bfloat16
BF16_MAX = float(jnp.finfo(jnp.bfloat16).max)
PEERS = [(2, 0), (2, 1), (1, 0), (3, 0), (1, 1), (3, 1), (0, 1)]
MATES = [1, 3, 2]


def div12(v):
    return (v * 2731) >> 15


def nt_dot(a, b):
    return lax.dot_general(a, b, (((1,), (1,)), ((), ())), preferred_element_type=F32)


def dot(a, b):
    return jnp.dot(a, b, preferred_element_type=F32)


def moe_kernel(
    n_line, cap, n_half, n_chunk, f_tile, cuts, ahead, lead, lag,
    x_hbm, idx_hbm, gate_hbm, w1_hbm, w3_hbm, w2_hbm, out_ref,
    x_ref, idx_ref, gate_ref, w1, w3, w2, slots, gates, mts, slots_far, gates_near, xg, sel, sendb, rows, part_a, part_b, hid, y1,
    y_raw, y_far, perm, gmat, acc, part_out, part_in,
    in_sem, w13_sem, w2_sem, mt_s, mt_r, n_s, n_r, g_s, g_r, d_s, d_r, c_s, c_r, e_s, e_r, f_r, p_s, p_r,
):
    n_tok, dim = x_ref.shape
    n_top = idx_ref.shape[0]
    n_loc, ffn = w2_hbm.shape[0], w2_hbm.shape[1]
    n_exp = slots.shape[0]
    n_line_exp = n_exp // n_line
    per = n_line * cap
    n_rows = 2 * n_line * per
    n_w2 = w2.shape[0]
    half = dim // n_half
    wide = dim // n_chunk

    dp = lax.axis_index('dp')
    yy = lax.axis_index('ep2')
    ee = lax.axis_index('ep')
    xx = ee // 2
    cc = lax.rem(ee, 2)
    k_self = jnp.where(cc == 0, yy, xx)
    q_self = jnp.where(cc == 0, xx, yy)
    i_self = cc * n_line + q_self
    d_self = 2 * q_self + cc
    coef_k = jnp.where(cc == 0, 16, 4)
    coef_q = jnp.where(cc == 0, 4, 16)

    def mod(v):
        return lax.rem(v + n_line, n_line)

    def mate(m):
        k = mod(k_self + m)
        return (dp, jnp.where(cc == 0, k, yy), jnp.where(cc == 0, xx, k) * 2 + cc)

    def spread_peer(m, dc):
        q = mod(q_self + m)
        c2 = lax.rem(cc + dc, 2)
        dev = (dp, jnp.where(cc == 0, yy, q), jnp.where(cc == 0, q, xx) * 2 + c2)
        return dev, 2 * q + c2

    def rows_at(start, size, unit):
        return pl.ds(pl.multiple_of(start, unit), size)

    def half_cols(h):
        return pl.ds(h * half, half)

    def cols_at(c):
        return pl.ds(pl.multiple_of(c * wide, wide), wide)

    def w13_copy(which, l):
        hbm, buf = ((w1_hbm, w1), (w3_hbm, w3))[which]
        return pltpu.make_async_copy(hbm.at[l], buf.at[l], w13_sem.at[which, l])

    def w2_copy(t):
        slot = lax.rem(t, n_w2)
        return pltpu.make_async_copy(
            w2_hbm.at[t // n_chunk, :, cols_at(lax.rem(t, n_chunk))], w2.at[slot], w2_sem.at[slot])

    def mt_copy(m):
        return pltpu.make_async_remote_copy(
            slots.at[line_rows(mod(k_self + m)), :], mts.at[k_self], mt_s.at[0], mt_r.at[0], device_id=mate(m), device_id_type=MESH)

    def gather_copy(m, h):
        return pltpu.make_async_remote_copy(
            x_ref.at[:, half_cols(h)], xg.at[rows_at(k_self * n_tok, n_tok, 8), half_cols(h)],
            g_s.at[0], g_r.at[m // 2, h], device_id=mate(m), device_id_type=MESH)

    def relay_copy(m, h):
        side = m // 2
        block = xg.at[rows_at(mod(k_self - m) * n_tok + side * (n_tok // 2), n_tok // 2, 8), half_cols(h)]
        return pltpu.make_async_remote_copy(
            block, block, g_s.at[0], g_r.at[2, h], device_id=mate(m), device_id_type=MESH)

    def wait_bytes(ref, sem):
        pltpu.make_async_copy(ref, ref, sem).wait()

    def spread_copy(l, h, m, dc):
        dev, d = spread_peer(m, dc)
        return pltpu.make_async_remote_copy(
            sendb.at[l, rows_at(d * per, per, 8), half_cols(h)],
            rows.at[l, rows_at(i_self * per, per, 8), half_cols(h)],
            d_s.at[0], d_r.at[l, group_of(l, h)], device_id=dev, device_id_type=MESH)

    others = (2 * n_line - 1) * per

    def group_of(l, h):
        return sum(h >= edge for edge in cuts[l])

    def spread_wait(l, h0, h1):
        wait_bytes(rows.at[l, pl.ds(0, others), pl.ds(h0 * half, (h1 - h0) * half)], d_r.at[l, group_of(l, h0)])

    def back_targets():
        out = []
        for m in (2, 1, 3):
            for side in (0, 1):
                pos = mod((yy if side else xx) + m)
                dev = (dp, pos, xx * 2 + 1) if side else (dp, yy, pos * 2)
                d_me = 2 * (yy if side else xx) + cc
                out.append((side * n_line + pos, dev, d_me))
        other = 1 - cc
        pos = jnp.where(other == 0, xx, yy)
        out.append((other * n_line + pos, (dp, yy, xx * 2 + other), 2 * pos + cc))
        return out

    def back_copies(l, c):
        return [
            pltpu.make_async_remote_copy(
                rows.at[l, rows_at(i * per, per, 8), cols_at(c)], y1.at[l, rows_at(d_me * per, per, 8), cols_at(c)],
                c_s.at[0], c_r.at[l, c], device_id=dev, device_id_type=MESH)
            for i, dev, d_me in back_targets()
        ]

    def back_wait(l, c):
        wait_bytes(y1.at[l, pl.ds(0, others), cols_at(c)], c_r.at[l, c])

    home = 2 * n_line * cap
    both = n_loc * home

    def at_home(s, l):
        return s >> 1, rows_at((s & 1) * both + l * home, home, 8)

    def side_cols(c, side):
        return pl.ds(pl.multiple_of(c * wide + side * (wide // 2), wide // 2), wide // 2)

    def raw_copy(l, c, m):
        side = m // 2
        p, r = at_home(mod(k_self + m), l)
        return pltpu.make_async_remote_copy(
            sendb.at[p, r, side_cols(c, side)], y_raw.at[pl.ds(l * home, home), side_cols(c, side)],
            e_s.at[0], e_r.at[c], device_id=mate(m), device_id_type=MESH)

    def far_copy(l, c, m):
        side = 1 - m // 2
        p, r = at_home(mod(k_self + 2), l)
        return pltpu.make_async_remote_copy(
            sendb.at[p, r, side_cols(c, side)], y_far.at[pl.ds(l * home, home), side_cols(c, side)],
            e_s.at[0], f_r.at[c], device_id=mate(m), device_id_type=MESH)

    def sum_copy(c, m):
        cols = side_cols(c, 1 - m // 2)
        return pltpu.make_async_remote_copy(
            part_out.at[:, cols], part_in.at[:, cols], p_s.at[0], p_r.at[c], device_id=mate(m), device_id_type=MESH)

    def line_rows(k):
        return pl.ds(pl.multiple_of(k * n_line_exp, n_line_exp), n_line_exp)

    def note_copies(m):
        side = m // 2
        out = [pltpu.make_async_remote_copy(
            slots.at[line_rows(mod(k_self + 2)), :], slots_far.at[side], n_s.at[0], n_r.at[0],
            device_id=mate(m), device_id_type=MESH)]
        for n, k in enumerate((mod(k_self + m), mod(k_self + 2))):
            out.append(pltpu.make_async_remote_copy(
                gates.at[line_rows(k), :], gates_near.at[side, n], n_s.at[1], n_r.at[1],
                device_id=mate(m), device_id_type=MESH))
        return out

    inputs = [
        pltpu.make_async_copy(src, dst, in_sem.at[n])
        for n, (src, dst) in enumerate(((idx_hbm, idx_ref), (x_hbm, x_ref), (gate_hbm, gate_ref)))
    ]
    for copy in inputs:
        copy.start()

    barrier = pltpu.get_barrier_semaphore()
    for side in (0, 1):
        for m in range(n_line):
            for dc in (0, 1):
                if (m, dc) == (0, 0) or (side and m == 0):
                    continue
                pos = mod((yy if side else xx) + m)
                c2 = lax.rem(cc + dc, 2)
                dev = (dp, pos, xx * 2 + c2) if side else (dp, yy, pos * 2 + c2)
                pl.semaphore_signal(barrier, inc=1, device_id=dev, device_id_type=MESH)

    for l in range(n_loc):
        for which in range(2):
            w13_copy(which, l).start()
    for t in range(n_w2):
        w2_copy(t).start()

    r_e = lax.broadcasted_iota(jnp.int32, (n_exp, n_tok), 0)
    row_e = (coef_k * (r_e >> 4) + coef_q * ((r_e >> 2) & 3) + (r_e & 3))
    inputs[0].wait()
    chosen = jnp.zeros((n_exp, n_tok), F32)
    for j in range(n_top):
        chosen = chosen + (idx_ref[j:j + 1, :] == row_e).astype(F32)
    before = (lax.broadcasted_iota(jnp.int32, (n_tok, n_tok), 0)
              < lax.broadcasted_iota(jnp.int32, (n_tok, n_tok), 1)).astype(BF16)
    slot = dot(chosen.astype(BF16), before)
    slot = jnp.where(chosen > 0, slot, -1.0).astype(BF16)
    slots[...] = slot
    mts[k_self] = slots[line_rows(k_self), :]

    inputs[2].wait()
    gate = jnp.zeros((n_exp, n_tok), F32)
    for j in range(n_top):
        gate = gate + jnp.where(idx_ref[j:j + 1, :] == row_e, gate_ref[j:j + 1, :], 0.0)
    gates[...] = gate

    with jax.named_scope('entry_wait'):
        pl.semaphore_wait(barrier, 4 * n_line - 3)

    inputs[1].wait()
    for m in MATES:
        mt_copy(m).start()
    for h in range(ahead):
        for m in (1, 3):
            gather_copy(m, h).start()

    xg[rows_at(k_self * n_tok, n_tok, 8), :] = x_ref[...]

    def relay(h):
        for m in (1, 3):
            gather_copy(m, h).wait_recv()
            relay_copy(m, h).start()

    relay(0)

    r = lax.broadcasted_iota(jnp.int32, (n_rows, 1), 0)
    r12 = div12(r)
    r_slot = (r - r12 * cap).astype(F32)
    r_src = r12 & (n_line - 1)
    r_dev = r12 >> 2
    e_lane = lax.broadcasted_iota(jnp.int32, (n_rows, n_line_exp), 1)
    with jax.named_scope('slots_wait'):
        wait_bytes(mts.at[pl.ds(0, n_line - 1)], mt_r.at[0])
    for l in range(n_loc):
        pick = (e_lane == n_loc * r_dev + l).astype(BF16)
        for s in range(n_line):
            val = dot(pick, mts[s])
            hit = jnp.logical_and(val == r_slot, r_src == s)
            sel[l, :, s * n_tok:(s + 1) * n_tok] = jnp.where(hit, 1.0, 0.0).astype(BF16)

    def spread(l, h):
        sendb[l, :, half_cols(h)] = dot(sel[l], xg[:, half_cols(h)]).astype(BF16)
        for m, dc in PEERS:
            spread_copy(l, h, m, dc).start()
        rows[l, rows_at(i_self * per, per, 8), half_cols(h)] = sendb[l, rows_at(d_self * per, per, 8), half_cols(h)]


    def gathered(h):
        with jax.named_scope('gather_wait'):
            wait_bytes(xg.at[pl.ds(0, n_tok), half_cols(h)], g_r.at[2, h])
        with jax.named_scope('spread_send'):
            spread(0, h)

    with jax.named_scope('gather_and_spread'):
        for h in range(n_half):
            if h > 0:
                relay(h)
            if h + ahead < n_half:
                for m in (1, 3):
                    gather_copy(m, h + ahead).start()
            if h >= lead - 1:
                gathered(h - lead + 1)
        for m in (1, 3):
            for copy in note_copies(m):
                copy.start()
        for h in range(n_half - lead + 1, n_half):
            gathered(h)

    with jax.named_scope('spread_rest'):
        for h in range(n_half):
            for l in range(1, n_loc):
                spread(l, h)

    o12 = r12
    o_in = (o12 & 7) * per + (o12 >> 3) * cap + (r - r12 * cap)
    perm[...] = (lax.broadcasted_iota(jnp.int32, (n_rows, n_rows), 1) == o_in).astype(BF16)

    acc[...] = x_ref[...].astype(F32)

    def expert_up(l, cuts):
        with jax.named_scope('weight_wait'):
            for which in range(2):
                w13_copy(which, l).wait()
        edges = (0,) + cuts + (n_half,)
        for h0, h1 in zip(edges, edges[1:]):
            with jax.named_scope('spread_wait'):
                spread_wait(l, h0, h1)
            k = slice(h0 * half, h1 * half)

            def tile(n, carry, h0=h0, h1=h1, k=k):
                cols = pl.ds(pl.multiple_of(n * f_tile, f_tile), f_tile)
                a = dot(rows[l, :, k], w1[l, k, cols])
                b = dot(rows[l, :, k], w3[l, k, cols])
                if h0 > 0:
                    a = a + part_a[:, cols]
                    b = b + part_b[:, cols]
                if h1 < n_half:
                    part_a[:, cols] = a
                    part_b[:, cols] = b
                else:
                    hid[:, cols] = (jax.nn.silu(a) * b).astype(BF16)
                return carry

            with jax.named_scope('up'):
                lax.fori_loop(0, ffn // f_tile, tile, 0)

    def expert_down(l, c):
        t = l * n_chunk + c
        w2_copy(t).wait()
        rows[l, :, cols_at(c)] = dot(hid[...], w2[lax.rem(t, n_w2)]).astype(BF16)

        @pl.when(t + n_w2 < n_loc * n_chunk)
        def _():
            w2_copy(t + n_w2).start()

        for copy in back_copies(l, c):
            copy.start()
        y1[l, rows_at(d_self * per, per, 8), cols_at(c)] = rows[l, rows_at(i_self * per, per, 8), cols_at(c)]

    def forward(l, c):
        with jax.named_scope('back_wait'):
            back_wait(l, c)
        out = dot(perm[...], y1[l, :, cols_at(c)]).astype(BF16)
        for s in range(n_line):
            sendb[s >> 1, (s & 1) * both + l * home:(s & 1) * both + (l + 1) * home, cols_at(c)] = (
                out[s * home:(s + 1) * home])
        for m in (1, 3):
            far_copy(l, c, m).start()
        for m in (1, 3):
            raw_copy(l, c, m).start()

    def fold(v):
        return v[:n_tok] + v[n_tok:2 * n_tok] + v[2 * n_tok:]

    def home_rows(s):
        return s >> 1, rows_at((s & 1) * both, both, 8)

    def own_sums(c):
        p, r = home_rows(k_self)
        acc[:, cols_at(c)] += fold(dot(gmat[0], sendb[p, r, cols_at(c)]))
        for side, m in ((0, 3), (1, 1)):
            p, r = home_rows(mod(k_self + m))
            part_out[:, side_cols(c, side)] = fold(
                dot(sel[side, :, 0:both], sendb[p, r, side_cols(c, side)]))

    def merge(c):
        with jax.named_scope('far_wait'):
            wait_bytes(y_far.at[:, cols_at(c)], f_r.at[c])
        for side in range(2):
            cols = side_cols(c, side)
            part_out[:, cols] += fold(dot(sel[side, :, 256:256 + both], y_far[:, cols]))
        for m in (1, 3):
            sum_copy(c, m).start()

    def collect(c):
        with jax.named_scope('raw_wait'):
            wait_bytes(y_raw.at[:, cols_at(c)], e_r.at[c])
        for side in range(2):
            cols = side_cols(c, side)
            acc[:, cols] += fold(dot(gmat[1 + side], y_raw[:, cols]))

    def loop(body, start=0, stop=n_chunk):
        def step(c, carry):
            body(c)
            return carry
        lax.fori_loop(start, stop, step, 0)

    expert_up(0, cuts[0])
    with jax.named_scope('down0'):
        loop(lambda c: expert_down(0, c))
    expert_up(1, cuts[1])
    with jax.named_scope('spread_drain'):
        wait_bytes(sendb.at[:, pl.ds(0, others), :], d_s.at[0])

    def down_and_forward(c):
        expert_down(1, c)
        forward(0, c)

    with jax.named_scope('down1_forward0'):
        loop(down_and_forward)

    with jax.named_scope('gate_blocks'):
        eye = (lax.broadcasted_iota(jnp.int32, (n_tok, n_tok), 0)
               == lax.broadcasted_iota(jnp.int32, (n_tok, n_tok), 1)).astype(BF16)
        q = lax.broadcasted_iota(jnp.int32, (1, both), 1)
        q12 = div12(q)
        q_slot = (q - q12 * cap).astype(F32)
        q_exp = n_loc * (q12 & 7) + (q12 >> 3)
        spread_e = (lax.broadcasted_iota(jnp.int32, (n_line_exp, both), 0) == q_exp).astype(BF16)

        def gate_block(slot_rows, gate_rows, put):
            hit = dot(nt_dot(eye, slot_rows).astype(BF16), spread_e) == q_slot
            rest = gate_rows
            for p in range(3):
                part = jnp.minimum(rest, BF16_MAX).astype(BF16)
                rest = rest - part.astype(F32)
                put(p, jnp.where(hit, dot(nt_dot(eye, part).astype(BF16), spread_e), 0.0).astype(BF16))

        for n, m in enumerate((0, 3, 1)):
            k = line_rows(mod(k_self + m))

            def put_own(p, v, n=n):
                gmat[n, p * n_tok:(p + 1) * n_tok, :] = v

            gate_block(slots[k, :], gates[k, :], put_own)
        wait_bytes(slots_far, n_r.at[0])
        wait_bytes(gates_near, n_r.at[1])
        for side in range(2):
            for n in range(2):
                near = mts[mod(k_self + (3 if side == 0 else 1))] if n == 0 else slots_far[side]

                def put_near(p, v, side=side, n=n):
                    sel[side, p * n_tok:(p + 1) * n_tok, n * 256:n * 256 + both] = v

                gate_block(near, gates_near[side, n], put_near)
    def forward_and_sum(c):
        forward(1, c)
        own_sums(c)

    def forward_and_merge(c):
        forward_and_sum(c)
        merge(c - lag)

    with jax.named_scope('forward1'):
        loop(forward_and_sum, 0, lag)
        loop(forward_and_merge, lag, n_chunk)

    def merge_and_collect(c):
        merge(c)
        collect(c - n_chunk + lag)

    with jax.named_scope('merge'):
        loop(merge_and_collect, n_chunk - lag, n_chunk)
        loop(collect, lag, n_chunk)
    wait_bytes(xg.at[pl.ds(0, (n_line - 1) * n_tok), :], g_s.at[0])

    def finish(c):
        with jax.named_scope('sum_wait'):
            wait_bytes(part_in.at[:, cols_at(c)], p_r.at[c])
        out_ref[:, cols_at(c)] = (acc[:, cols_at(c)] + part_in[:, cols_at(c)]).astype(BF16)

    with jax.named_scope('finish'):
        loop(finish)

    with jax.named_scope('drain'):
        wait_bytes(mts.at[pl.ds(0, n_line - 1)], mt_s.at[0])
        wait_bytes(slots_far, n_s.at[0])
        wait_bytes(gates_near, n_s.at[1])
        wait_bytes(y1.at[:, pl.ds(0, others), :], c_s.at[0])
        wait_bytes(y1.at[0], e_s.at[0])
        wait_bytes(part_out, p_s.at[0])


def solution(mesh):
    group_axes = ('ep2', 'ep')
    n_line = mesh.shape['ep2']
    n_group = n_line * mesh.shape['ep']
    row_spec = P(('dp', 'ep2', 'ep'), None)
    weight_spec = P(group_axes, None, None)

    def device_step(tokens, expert_ids, gates, w_gate, w_up, w_down):
        n_tok, n_top = expert_ids.shape
        n_loc, dim, ffn = w_gate.shape
        n_exp = n_loc * n_group
        cap = -(-(n_tok * n_top) // n_exp)
        n_rows = n_group * cap
        n_half, n_chunk, f_tile, n_w2, cuts, ahead, lead, lag = 5, 5, 256, 3, ((2, 4), (2, 4)), 4, 3, 3
        sem = pltpu.SemaphoreType.DMA
        hbm = pl.BlockSpec(memory_space=pl.ANY)
        n_dev = 2 * n_line
        return pl.pallas_call(
            functools.partial(moe_kernel, n_line, cap, n_half, n_chunk, f_tile, cuts, ahead, lead, lag),
            out_shape=pltpu.VMEM((n_tok, dim), BF16),
            in_specs=[hbm] * 6,
            out_specs=pl.BlockSpec(memory_space=pltpu.VMEM),
            scratch_shapes=[
                pltpu.VMEM((n_tok, dim), BF16),
                pltpu.VMEM((n_top, n_tok), jnp.int32),
                pltpu.VMEM((n_top, n_tok), F32),
                pltpu.VMEM((n_loc, dim, ffn), BF16),
                pltpu.VMEM((n_loc, dim, ffn), BF16),
                pltpu.VMEM((n_w2, ffn, dim // n_chunk), BF16),
                pltpu.VMEM((n_exp, n_tok), BF16),
                pltpu.VMEM((n_exp, n_tok), F32),
                pltpu.VMEM((n_line, n_exp // n_line, n_tok), BF16),
                pltpu.VMEM((2, n_exp // n_line, n_tok), BF16),
                pltpu.VMEM((2, 2, n_exp // n_line, n_tok), F32),
                pltpu.VMEM((n_line * n_tok, dim), BF16),
                pltpu.VMEM((n_loc, n_rows, n_line * n_tok), BF16),
                pltpu.VMEM((n_loc, n_rows, dim), BF16),
                pltpu.VMEM((n_loc, n_rows, dim), BF16),
                pltpu.VMEM((n_rows, ffn), F32),
                pltpu.VMEM((n_rows, ffn), F32),
                pltpu.VMEM((n_rows, ffn), BF16),
                pltpu.VMEM((n_loc, n_rows, dim), BF16),
                pltpu.VMEM((n_loc * n_dev * cap, dim), BF16),
                pltpu.VMEM((n_loc * n_dev * cap, dim), BF16),
                pltpu.VMEM((n_rows, n_rows), BF16),
                pltpu.VMEM((3, 3 * n_tok, n_loc * n_dev * cap), BF16),
                pltpu.VMEM((n_tok, dim), F32),
                pltpu.VMEM((n_tok, dim), F32),
                pltpu.VMEM((n_tok, dim), F32),
                sem((3,)),
                sem((2, n_loc)),
                sem((n_w2,)),
                sem((1,)), sem((1,)),
                sem((2,)), sem((2,)),
                sem((1,)), sem((3, n_half)),
                sem((1,)), sem((n_loc, 1 + max(len(edges) for edges in cuts))),
                sem((1,)), sem((n_loc, n_chunk)),
                sem((1,)), sem((n_chunk,)), sem((n_chunk,)),
                sem((1,)), sem((n_chunk,)),
            ],
            compiler_params=pltpu.CompilerParams(
                collective_id=0, has_side_effects=True, vmem_limit_bytes=66300000),
        )(tokens, expert_ids.T, gates.T, w_gate, w_up, w_down)

    return jax.shard_map(
        device_step, mesh=mesh,
        in_specs=(row_spec, row_spec, row_spec, weight_spec, weight_spec, weight_spec),
        out_specs=row_spec, check_vma=False)
```
